32 devices in a mesh: row: 4 (over y, x), col: 8 (over z, core).
Axes of the slice: x: 2, y: 2, z: 4, core: 2. Of those that a mesh axis runs over, the one named last changes fastest.
Arguments:
- initial_field: float32 [1, 512, 4096], P(None, 'row', 'col'), may hold values from -12 to 12
- information: float32 [512, 4096], P('row', 'col'), may hold values from -24 to 24
- kappa_squared: float32 [512, 4096], P('row', 'col'), may hold values from 0.05 to 2
- lumped_mass: float32 [512, 4096], P('row', 'col'), may hold values from 0.5 to 2
- noise_seeds: int32 [4, 8, 2, 4, 1], P('row', 'col'), may hold values from 0 to 1073741823
- colour_order: int32 [4], replicated, may hold values from 0 to 3, each once
Outputs:
- final_field: float32 [1, 512, 4096], P(None, 'row', 'col')
- energies: float32 [2, 4, 1], replicated
The draws below stay inside these ranges and needn't reach their ends.
Inputs may be any that keep to these rules, and one draw needn't show every extreme that they name: `noise_seeds`: one seed for each tile of 128 x 512 nodes, sweep, colour phase and chain. `colour_order`: names each of the 4 block colours once.
All inputs are finite; a program needn't handle non-finite values.
Results may differ from the reference program's by a relative error of at most 0.0003.
Values sent between devices are 32-bit elements; how exact they have to be, the bound alone decides.
No kernel may reach another device: no remote copies, remote signals or barrier semaphores. Data moves between devices by JAX's collectives and lax.ppermute only.
A program may use at most 128 MiB of HBM per device.

```python
import math
import jax
import jax.numpy as jnp
from jax import lax

TR = 128
TC = 512
CHAINS = 1
SWEEPS = 2
COLOURS = 4
NR = 512
NC = 4096
ROW_TILES = 4
COL_TILES = 8


def ramp_scale():
    down_axis = jnp.arange(NR, dtype=jnp.float32) / NR
    across = jnp.arange(NC, dtype=jnp.float32) / NC
    return 1.0 + down_axis[:, None] + across[None, :]


def draw_initial_field(key, part):
    key = jax.random.fold_in(key, 17)
    values = jnp.clip(jax.random.normal(key, (CHAINS, NR, NC), jnp.float32), -4.0, 4.0)
    return values * ramp_scale()


def draw_information(key, part):
    key = jax.random.fold_in(key, 29)
    values = 2.0 * jnp.clip(jax.random.normal(key, (NR, NC), jnp.float32), -4.0, 4.0)
    return values * ramp_scale()


def plant(array, rng, least, largest):
    place = [jax.random.randint(jax.random.fold_in(rng, axis), (), 0, length) for axis, length in enumerate(array.shape)]
    longest = array.shape.index(max(array.shape))
    beside = place[:longest] + [(place[longest] + 1) % array.shape[longest]] + place[longest + 1:]
    return array.at[tuple(place)].set(least).at[tuple(beside)].set(largest)


def level_of(own_key, extent, split, smallest, largest):
    def one(axis_at, shards_of):
        steps = jax.random.uniform(jax.random.fold_in(jax.random.fold_in(own_key, 6), axis_at), (shards_of,), jnp.float32, smallest / len(split), largest / len(split))
        return jnp.repeat(jnp.exp(steps), extent[axis_at] // shards_of).reshape((-1,) + (1,) * (len(extent) - axis_at - 1))

    factor_of = one(*split[0])
    for cut in split[1:]:
        factor_of = factor_of * one(*cut)
    return factor_of


def setup_inputs(seed: int = 0) -> dict:
    keys = jax.random.split(jax.random.key(seed), 7)
    return {
        "initial_field": draw_initial_field(jax.random.fold_in(keys[6], 71), 0),
        "information": draw_information(jax.random.fold_in(keys[6], 71), 0),
        "kappa_squared": jnp.clip(jnp.exp(math.log(2.0) - 3.6888794 * jax.random.uniform(keys[2], (NR, NC), jnp.float32) ** level_of(keys[2], (NR, NC), ((0, 4), (1, 8)), -0.2, 0.2)), 0.05, 2.0),
        "lumped_mass": jnp.clip(jnp.exp(math.log(2.0) - 1.3862944 * jax.random.uniform(keys[3], (NR, NC), jnp.float32) ** level_of(keys[3], (NR, NC), ((0, 4), (1, 8)), -0.2, 0.2)), 0.5, 2.0),
        "noise_seeds": plant(jax.random.randint(keys[4], (ROW_TILES, COL_TILES, SWEEPS, COLOURS, CHAINS), 0, 1073741824), jax.random.fold_in(keys[4], 1), 0, 1073741823).astype(jnp.int32),
        "colour_order": jax.random.permutation(keys[5], COLOURS).astype(jnp.int32),
    }


full_turn = 6.283185307179586
unit_step = 1.0 / 8388608.0
mix_factor = 73244475

def neighbours(source):
    return jnp.roll(source, 1, axis=-2) + jnp.roll(source, -1, axis=-2) + jnp.roll(source, 1, axis=-1) + jnp.roll(source, -1, axis=-1)

def apply_precision(sample_field, stiffness, inverse):
    first_pass = stiffness * sample_field - neighbours(sample_field)
    scaled = inverse * first_pass
    return stiffness * scaled - neighbours(scaled)

def corners(source):
    leading = source.shape[:-2]
    height, breadth = (source.shape[-2], source.shape[-1])
    shaped = source.reshape(leading + (height // 2, 2, breadth // 2, 2))
    return [shaped[..., :, first_index, :, second_index] for first_index in (0, 1) for second_index in (0, 1)]

def join_corners(pieces):
    top_half = jnp.stack([pieces[0], pieces[1]], axis=-1)
    bottom_half = jnp.stack([pieces[2], pieces[3]], axis=-1)
    top_half = top_half.reshape(top_half.shape[:-2] + (top_half.shape[-2] * 2,))
    bottom_half = bottom_half.reshape(bottom_half.shape[:-2] + (bottom_half.shape[-2] * 2,))
    stacked = jnp.stack([top_half, bottom_half], axis=-2)
    return stacked.reshape(stacked.shape[:-3] + (stacked.shape[-3] * 2, stacked.shape[-1]))

def block_matrix(stiff_corners, inverse_corners, diagonal_corners):
    scaled = [stiff_corners[corner] * inverse_corners[corner] for corner in range(4)]
    matrix = [[None] * 4 for corner in range(4)]
    for corner in range(4):
        matrix[corner][corner] = diagonal_corners[corner]
    for first_index, second_index in ((0, 1), (0, 2), (1, 3), (2, 3)):
        element = -(scaled[first_index] + scaled[second_index])
        matrix[first_index][second_index] = element
        matrix[second_index][first_index] = element
    matrix[0][3] = inverse_corners[1] + inverse_corners[2]
    matrix[3][0] = matrix[0][3]
    matrix[1][2] = inverse_corners[0] + inverse_corners[3]
    matrix[2][1] = matrix[1][2]
    return matrix

def cholesky_rows(matrix):
    factor = [[None] * 4 for corner in range(4)]
    for first_index in range(4):
        for second_index in range(first_index + 1):
            running = matrix[first_index][second_index]
            for middle in range(second_index):
                running = running - factor[first_index][middle] * factor[second_index][middle]
            if first_index == second_index:
                factor[first_index][first_index] = jnp.sqrt(running)
            else:
                factor[first_index][second_index] = running / factor[second_index][second_index]
    return factor

def resample(field_corners, applied_corners, info_corners, matrix, factor, noise_list):
    right_side = []
    for first_index in range(4):
        coupled = matrix[first_index][0] * field_corners[0]
        for second_index in range(1, 4):
            coupled = coupled + matrix[first_index][second_index] * field_corners[second_index]
        right_side.append(info_corners[first_index] - applied_corners[first_index] + coupled)
    forward = []
    for first_index in range(4):
        running = right_side[first_index]
        for second_index in range(first_index):
            running = running - factor[first_index][second_index] * forward[second_index]
        forward.append(running / factor[first_index][first_index])
    shifted = [forward[corner] + noise_list[corner] for corner in range(4)]
    result = [None] * 4
    for first_index in reversed(range(4)):
        running = shifted[first_index]
        for second_index in range(first_index + 1, 4):
            running = running - factor[second_index][first_index] * result[second_index]
        result[first_index] = running / factor[first_index][first_index]
    return result

def scramble(hashed):
    sixteen = jnp.full_like(hashed, 16)
    hashed = hashed ^ lax.shift_right_logical(hashed, sixteen)
    hashed = hashed * mix_factor
    hashed = hashed ^ lax.shift_right_logical(hashed, sixteen)
    hashed = hashed * mix_factor
    return hashed ^ lax.shift_right_logical(hashed, sixteen)

def gaussian(seed_nodes, offsets):
    first_hash = scramble(seed_nodes + 2 * offsets)
    second_hash = scramble(seed_nodes + 2 * offsets + 1)
    shift_nine = jnp.full_like(first_hash, 9)
    uniform_one = (lax.shift_right_logical(first_hash, shift_nine).astype(jnp.float32) + 1.0) * unit_step
    uniform_two = lax.shift_right_logical(second_hash, shift_nine).astype(jnp.float32) * unit_step
    return jnp.sqrt(-2.0 * jnp.log(uniform_one)) * jnp.cos(full_turn * uniform_two)

def reference(initial_field, information, kappa_squared, lumped_mass, noise_seeds, colour_order):
    stiffness = kappa_squared * lumped_mass + 4.0
    inverse = 1.0 / lumped_mass
    diagonal = stiffness * stiffness * inverse + neighbours(inverse)
    matrix = block_matrix(corners(stiffness), corners(inverse), corners(diagonal))
    factor = cholesky_rows(matrix)
    info_corners = corners(information)
    half_rows = jnp.arange(NR // 2, dtype=jnp.int32)
    half_cols = jnp.arange(NC // 2, dtype=jnp.int32)
    block_colour = 2 * (half_rows % 2)[:, None] + (half_cols % 2)[None, :]
    offset_list = []
    tile_list = []
    for corner in range(4):
        node_rows = 2 * half_rows + corner // 2
        node_cols = 2 * half_cols + corner % 2
        offset_list.append((node_rows % TR)[:, None] * TC + (node_cols % TC)[None, :])
        tile_list.append((node_rows // TR, node_cols // TC))

    def one_sweep(sweep_index, loop_state):
        sample_field, energies = loop_state
        seed_layer = lax.dynamic_index_in_dim(noise_seeds, sweep_index, 2, keepdims=False)
        for phase_index in range(COLOURS):
            applied = apply_precision(sample_field, stiffness, inverse)
            energy = lax.optimization_barrier(jnp.sum(0.5 * sample_field * applied - information * sample_field, axis=(1, 2))) / (NR * NC)
            energies = energies.at[sweep_index, phase_index].set(energy)
            seed_table = seed_layer[:, :, phase_index, :]
            noise_list = []
            for corner in range(4):
                picked = seed_table[tile_list[corner][0]][:, tile_list[corner][1]]
                noise_list.append(gaussian(jnp.moveaxis(picked, -1, 0), offset_list[corner]))
            before = corners(sample_field)
            updated = resample(before, corners(applied), info_corners, matrix, factor, noise_list)
            chosen = block_colour == colour_order[phase_index]
            sample_field = join_corners([jnp.where(chosen, updated[corner], before[corner]) for corner in range(4)])
        return (sample_field, energies)
    initial = (initial_field, jnp.zeros((SWEEPS, COLOURS, CHAINS), jnp.float32))
    final_field, energies = lax.fori_loop(0, SWEEPS, one_sweep, initial)
    return (final_field, energies)
```

```python
import functools

import jax
import jax.numpy as jnp
from jax import lax
from jax.experimental import pallas as pl
from jax.experimental.pallas import tpu as pltpu
from jax.sharding import PartitionSpec as P

SWEEPS = 2
COLOURS = 4
PHASES = SWEEPS * COLOURS
HALO = 2 * PHASES
CELL = 4
HC = HALO // CELL
LANES = 128
SUB = 8
GROUP = LANES // CELL
AXES = ("row", "col")
F32 = jnp.float32
I32 = jnp.int32

unit_step = 1.0 / 8388608.0
mix_factor = 73244475
SEED_BASE = 32768

SIN_COEFFS = (
    6.283185306485777,
    -41.34170192921984,
    81.60520938153618,
    -76.70366601553475,
    41.99996083008805,
    -14.336855962945094,
)


def lane_iota(shape):
    return lax.broadcasted_iota(I32, shape, len(shape) - 1)


def sub_iota(shape):
    return lax.broadcasted_iota(I32, shape, len(shape) - 2)


def lane_gather(value, index):
    return jnp.take_along_axis(value, index, axis=1, mode="promise_in_bounds")


def lroll(value, amount):
    amount = amount % value.shape[1]
    return pltpu.roll(value, amount, 1) if amount else value


def seed_tile(seeds_ref):
    lane = lane_iota((SUB, LANES))
    tile = jnp.zeros((SUB, LANES), I32)
    for phase in range(PHASES):
        seed = seeds_ref[0, 0, phase // COLOURS, phase % COLOURS, 0]
        tile = jnp.where(lane == phase, seed // SEED_BASE, tile)
        tile = jnp.where(lane == PHASES + phase, seed % SEED_BASE, tile)
    return tile.astype(F32)


def pack_kernel(seeds_ref, *refs):
    sources, (up_ref, down_ref, left_ref, right_ref) = refs[:4], refs[4:]
    rows, cols = sources[0].shape
    lane = lane_iota((SUB, LANES))
    per = LANES // HALO
    for a, source in enumerate(sources):
        for edge, out in ((0, left_ref), (1, right_ref)):
            for v in range(rows // (SUB * per)):
                packed = jnp.zeros((SUB, LANES), F32)
                for q in range(per):
                    top = SUB * (v * per + q)
                    start = (cols - LANES) if edge else 0
                    piece = source[top : top + SUB, start : start + LANES]
                    offset = HALO * q - (LANES - HALO if edge else 0)
                    piece = lroll(piece, offset)
                    packed = jnp.where(lane // HALO == q, piece, packed)
                out[a * HALO + SUB * v : a * HALO + SUB * (v + 1), :] = packed
        up_ref[a * HALO : (a + 1) * HALO, :] = source[0:HALO, :]
        down_ref[a * HALO : (a + 1) * HALO, :] = source[rows - HALO : rows, :]
    seeds = seed_tile(seeds_ref)
    base = 4 * HALO
    for out in (up_ref, down_ref, left_ref, right_ref):
        out[base : base + SUB, 0:LANES] = seeds


def corner_kernel(right_ref, left_ref, up_ref, down_ref):
    lane = lane_iota((SUB, LANES))
    for a in range(4):
        for out, top, shift in ((up_ref, 0, 0), (down_ref, HALO - SUB, 2 * HALO)):
            r = right_ref[a * HALO + top : a * HALO + top + SUB, :]
            l = left_ref[a * HALO + top : a * HALO + top + SUB, :]
            r = lroll(r, shift)
            l = lroll(l, shift + 2 * HALO)
            out[a * SUB : (a + 1) * SUB, :] = jnp.where(lane < 2 * HALO, r, l)
    for out in (up_ref, down_ref):
        out[4 * SUB : 5 * SUB, :] = right_ref[4 * HALO : 4 * HALO + SUB, :]
        out[5 * SUB : 6 * SUB, :] = left_ref[4 * HALO : 4 * HALO + SUB, :]


def scramble(hashed):
    sixteen = jnp.full_like(hashed, 16)
    hashed = hashed ^ lax.shift_right_logical(hashed, sixteen)
    hashed = hashed * mix_factor
    hashed = hashed ^ lax.shift_right_logical(hashed, sixteen)
    hashed = hashed * mix_factor
    return hashed ^ lax.shift_right_logical(hashed, sixteen)


def gaussian(first):
    nine = jnp.full_like(first, 9)
    one = lax.shift_right_logical(scramble(first), nine).astype(F32)
    two = lax.shift_right_logical(scramble(first + 1), nine).astype(F32)
    u1 = (one + 1.0) * unit_step
    v = 0.25 - jnp.abs(two * unit_step - 0.5)
    square = v * v
    poly = jnp.full_like(v, SIN_COEFFS[-1])
    for coeff in SIN_COEFFS[-2::-1]:
        poly = poly * square + coeff
    return jnp.sqrt(-2.0 * jnp.log(u1)) * (-(v * poly))


def shifted(value, rows, cols):
    if rows:
        value = pltpu.roll(value, (-rows) % value.shape[0], 0)
    if cols:
        value = pltpu.roll(value, (-cols) % value.shape[1], 1)
    return value


def locate(r, c):
    return (r % CELL) * CELL + c % CELL, r // CELL, c // CELL


def fetch(ref, r, c):
    plane, rows, cols = locate(r, c)
    return shifted(ref[plane], rows, cols)


def neighbour_sum(ref, r, c):
    return (
        fetch(ref, r - 1, c) + fetch(ref, r + 1, c) + fetch(ref, r, c - 1) + fetch(ref, r, c + 1)
    )


def fold(value):
    total = value[0:SUB]
    for top in range(SUB, value.shape[0], SUB):
        total = total + value[top : top + SUB]
    return total


def block_nodes(colour):
    r0, c0 = 2 * (colour // 2), 2 * (colour % 2)
    return [(r0, c0), (r0, c0 + 1), (r0 + 1, c0), (r0 + 1, c0 + 1)]


def main_kernel(
    tile_rows, tile_cols, nodes,
    order_ref, seeds_ref, x_ref, b_ref, kappa_ref, mass_ref,
    below_ref, above_ref, right_ref, left_ref, cbelow_ref, cabove_ref,
    out_ref, energy_ref,
    nat, X, W, S, I, B, LM, Z, EN, ST,
):
    mr = tile_rows // CELL
    er = mr + 2 * HC
    tiles = tile_cols // LANES
    lane = lane_iota((SUB, LANES))
    sub = sub_iota((SUB, LANES))
    per = LANES // HALO
    edge = tiles

    for a, source in enumerate((x_ref, b_ref, kappa_ref, mass_ref)):
        for t in range(tiles):
            lanes = slice(t * LANES, (t + 1) * LANES)
            page = a * (tiles + 1) + t
            nat[page, 0:tile_rows, :] = source[:, lanes]
            nat[page, tile_rows : tile_rows + HALO, :] = below_ref[a * HALO : (a + 1) * HALO, lanes]
            nat[page, tile_rows + HALO : tile_rows + 2 * HALO, :] = above_ref[
                a * HALO : (a + 1) * HALO, lanes
            ]
        page = a * (tiles + 1) + edge

        def put(top, right, left):
            nat[page, top : top + SUB, :] = jnp.where(
                lane < HALO, right, jnp.where(lane >= LANES - HALO, left, 1.0)
            )

        for g in range(tile_rows // SUB):
            v, q = g // per, g % per
            rows = slice(a * HALO + SUB * v, a * HALO + SUB * (v + 1))
            put(
                SUB * g,
                lroll(right_ref[rows, :], -HALO * q),
                lroll(left_ref[rows, :], LANES - HALO - HALO * q),
            )
        for start, corner in ((tile_rows, cbelow_ref), (tile_rows + HALO, cabove_ref)):
            value = corner[a * SUB : (a + 1) * SUB, :]
            for h in range(HALO // SUB):
                put(
                    start + SUB * h,
                    lroll(value, -HALO * h),
                    lroll(value, LANES - HALO - 2 * HALO - HALO * h),
                )

    wide = lane_iota((er, LANES))
    group = wide // GROUP
    into = [CELL * (wide % GROUP) + (group + CELL - t) % CELL for t in range(CELL)]
    halo_index = [CELL * (wide % GROUP) + c for c in range(CELL)]

    def planes(a, r):
        page = a * (tiles + 1)
        pieces = [
            lane_gather(nat[page + t, pl.ds(r, er, stride=CELL), :], into[t]) for t in range(CELL)
        ]
        outer = nat[page + edge, pl.ds(r, er, stride=CELL), :]
        result = []
        for c in range(CELL):
            value = pieces[(-c) % CELL]
            for g in range(1, CELL):
                value = jnp.where(group == g, pieces[(g - c) % CELL], value)
            result.append((lroll(value, -GROUP * c), lane_gather(outer, halo_index[c])))
        return result

    for r in range(CELL):
        for c, (inner, outer) in enumerate(planes(0, r)):
            X[r * CELL + c, :, 0:LANES] = inner
            X[r * CELL + c, :, LANES : 2 * LANES] = outer
        for c, (inner, outer) in enumerate(planes(1, r)):
            B[r * CELL + c, :, 0:LANES] = inner
            B[r * CELL + c, :, LANES : 2 * LANES] = outer
        both = zip(planes(2, r), planes(3, r))
        for c, (kappas, masses) in enumerate(both):
            for half in range(2):
                lanes = slice(half * LANES, (half + 1) * LANES)
                S[r * CELL + c, :, lanes] = kappas[half] * masses[half] + 4.0
                I[r * CELL + c, :, lanes] = 1.0 / masses[half]

    energy = jnp.zeros((SUB, LANES), F32)
    for r in range(CELL):
        for c in range(CELL):
            plane = r * CELL + c
            field = X[plane]
            first = S[plane] * field - neighbour_sum(X, r, c)
            scaled = I[plane] * first
            W[plane] = scaled
            energy = energy + fold(
                (0.5 * scaled * first - B[plane] * field)[0:mr, 0:LANES]
            )
    EN[0] = energy

    for colour in range(COLOURS):
        nodes_here = block_nodes(colour)
        inv = [I[r * CELL + c] for r, c in nodes_here]
        stiff = [S[r * CELL + c] for r, c in nodes_here]
        scaled = [stiff[n] * inv[n] for n in range(4)]
        diag = [
            stiff[n] * scaled[n] + neighbour_sum(I, *nodes_here[n]) for n in range(4)
        ]
        m01, m02 = -(scaled[0] + scaled[1]), -(scaled[0] + scaled[2])
        m13, m23 = -(scaled[1] + scaled[3]), -(scaled[2] + scaled[3])
        m03, m12 = inv[1] + inv[2], inv[0] + inv[3]
        r0 = lax.rsqrt(diag[0])
        l10, l20, l30 = m01 * r0, m02 * r0, m03 * r0
        r1 = lax.rsqrt(diag[1] - l10 * l10)
        l21, l31 = (m12 - l20 * l10) * r1, (m13 - l30 * l10) * r1
        r2 = lax.rsqrt(diag[2] - l20 * l20 - l21 * l21)
        l32 = (m23 - l30 * l20 - l31 * l21) * r2
        r3 = lax.rsqrt(diag[3] - l30 * l30 - l31 * l31 - l32 * l32)
        for n, value in enumerate((r0, r1, r2, r3, l10, l20, l30, l21, l31, l32)):
            LM[colour * 10 + n] = value

    def whole(ref, top):
        tile = ref[top : top + SUB, 0:LANES].astype(I32)
        return (tile * SEED_BASE + lroll(tile, LANES - PHASES))[0:1, :]

    base = 4 * HALO
    around = {
        "B": whole(below_ref, base), "T": whole(above_ref, base),
        "R": whole(right_ref, base), "L": whole(left_ref, base),
        "BR": whole(cbelow_ref, 4 * SUB), "BL": whole(cbelow_ref, 5 * SUB),
        "TR": whole(cabove_ref, 4 * SUB), "TL": whole(cabove_ref, 5 * SUB),
    }
    spot = lane % GROUP
    low = sub < HC
    for phase in range(PHASES):
        pick = {
            key: jnp.broadcast_to(value[:, phase : phase + 1], (SUB, LANES))
            for key, value in around.items()
        }
        ST[phase, 0] = jnp.where(low, pick["B"], pick["T"])
        side = jnp.where(spot < GROUP // 2, pick["R"], pick["L"])
        corner_right = jnp.where(low, pick["BR"], pick["TR"])
        corner_left = jnp.where(low, pick["BL"], pick["TL"])
        side = jnp.where((lane >= 2 * HC) & (lane < 3 * HC), corner_right, side)
        side = jnp.where((lane >= HC) & (lane < 2 * HC), corner_left, side)
        ST[phase, 1] = side

    node_row = 2 * CELL * tile_cols
    node_col = 2 * CELL
    offset_main = node_row * sub_iota((mr, LANES)) + node_col * lane_iota((mr, LANES))
    strip_cell = jnp.where(low, sub, sub + mr - 2 * HC)
    offset_strip = node_row * strip_cell + node_col * lane
    side_group = jnp.where(spot < GROUP // 2, lane // GROUP, (lane // GROUP + 1) % CELL)
    side_row = SUB * side_group + sub
    side_col = jnp.where(spot < GROUP // 2, spot, spot + LANES - GROUP)
    in_corner = (lane >= HC) & (lane < 3 * HC)
    side_row = jnp.where(in_corner, strip_cell, side_row)
    side_col = jnp.where(
        in_corner, jnp.where(lane >= 2 * HC, lane - 2 * HC, lane + LANES - 2 * HC), side_col
    )
    offset_side = node_row * side_row + node_col * side_col

    def noise_phase(phase, carry):
        colour = order_ref[phase % COLOURS]
        r0, c0 = 2 * (colour // 2), 2 * (colour % 2)
        own = seeds_ref[0, 0, phase // COLOURS, phase % COLOURS, 0]
        strip_seed = ST[phase, 0]
        side_seed = ST[phase, 1]
        for n in range(4):
            extra = 2 * ((r0 + n // 2) * tile_cols + c0 + n % 2)
            at = phase * 4 + n
            Z[at, 0:mr, 0:LANES] = gaussian(offset_main + (own + extra))
            Z[at, mr:er, 0:LANES] = gaussian(offset_strip + strip_seed + extra)
            side = gaussian(offset_side + side_seed + extra)
            for g in range(mr // SUB):
                Z[at, SUB * g : SUB * (g + 1), LANES : 2 * LANES] = lroll(side, -GROUP * g)
            Z[at, mr:er, LANES : 2 * LANES] = lroll(side, -2 * HC)
        return carry

    lax.fori_loop(0, PHASES, noise_phase, 0)

    def phase_body(colour, phase):
        nodes_here = block_nodes(colour)
        r0, c0 = nodes_here[0]
        own = [r * CELL + c for r, c in nodes_here]
        w = {}
        for r in range(r0 - 1, r0 + 3):
            for c in range(c0 - 1, c0 + 3):
                inside_row, inside_col = r0 <= r <= r0 + 1, c0 <= c <= c0 + 1
                if inside_row or inside_col:
                    w[r, c] = fetch(W, r, c)
        residual = []
        for n, (r, c) in enumerate(nodes_here):
            around_sum = w[r - 1, c] + w[r + 1, c] + w[r, c - 1] + w[r, c + 1]
            residual.append(B[own[n]] - (S[own[n]] * w[r, c] - around_sum))
        q0, q1, q2, q3, l10, l20, l30, l21, l31, l32 = [LM[colour * 10 + n] for n in range(10)]
        z = [Z[phase * 4 + n] for n in range(4)]
        f0 = residual[0] * q0
        f1 = (residual[1] - l10 * f0) * q1
        f2 = (residual[2] - l20 * f0 - l21 * f1) * q2
        f3 = (residual[3] - l30 * f0 - l31 * f1 - l32 * f2) * q3
        y0, y1, y2, y3 = f0 + z[0], f1 + z[1], f2 + z[2], f3 + z[3]
        d3 = y3 * q3
        d2 = (y2 - l32 * d3) * q2
        d1 = (y1 - l21 * d2 - l31 * d3) * q1
        d0 = (y0 - l10 * d1 - l20 * d2 - l30 * d3) * q0
        change = jnp.zeros((SUB, LANES), F32)
        for n, f in enumerate((f0, f1, f2, f3)):
            zi, fi = z[n][0:mr, 0:LANES], f[0:mr, 0:LANES]
            change = change + fold(zi * zi - fi * fi)
        EN[phase + 1] = 0.5 * change
        delta = [d0, d1, d2, d3]
        for n in range(4):
            X[own[n]] = X[own[n]] + delta[n]
        for n, (across, down) in enumerate(((1, 2), (0, 3), (3, 0), (2, 1))):
            step = S[own[n]] * delta[n] - (delta[across] + delta[down])
            W[own[n]] = w[nodes_here[n]] + I[own[n]] * step
        for n, (r, c) in enumerate(nodes_here):
            for rr, cc in ((r - 1 if r == r0 else r + 1, c), (r, c - 1 if c == c0 else c + 1)):
                plane, rows, cols = locate(rr, cc)
                W[plane] = W[plane] - I[plane] * shifted(delta[n], -rows, -cols)

    def run_phase(phase, carry):
        colour = order_ref[phase % COLOURS]
        for option in range(COLOURS):
            @pl.when(colour == option)
            def _():
                phase_body(option, phase)
        return carry

    lax.fori_loop(0, PHASES, run_phase, 0)

    running = EN[0]
    result = jnp.zeros((1, LANES), F32)
    first_row = lane_iota((1, LANES))
    for phase in range(PHASES):
        if phase:
            running = running + EN[phase]
        total = jnp.sum(jnp.sum(running, axis=0, keepdims=True), axis=1, keepdims=True)
        result = jnp.where(first_row == phase, total, result)
    energy_ref[...] = jnp.broadcast_to(result / nodes, energy_ref.shape)

    tall = lane_iota((mr, LANES))
    group_out = tall // GROUP
    back = [GROUP * ((tall % CELL + t) % CELL) + tall // CELL for t in range(CELL)]
    for r in range(CELL):
        turned = [lroll(X[r * CELL + c, 0:mr, 0:LANES], GROUP * c) for c in range(CELL)]
        for t in range(tiles):
            value = turned[(-t) % CELL]
            for g in range(1, CELL):
                value = jnp.where(group_out == g, turned[(g - t) % CELL], value)
            nat[t, pl.ds(r, mr, stride=CELL), :] = lane_gather(value, back[t])
    for t in range(tiles):
        out_ref[:, t * LANES : (t + 1) * LANES] = nat[t, 0:tile_rows, :]


def ring(count, step):
    return [(i, (i + step) % count) for i in range(count)]


def local(initial_field, information, kappa_squared, lumped_mass, noise_seeds, colour_order):
    chains, tile_rows, tile_cols = initial_field.shape
    row_count, col_count = lax.axis_size("row"), lax.axis_size("col")
    devices = row_count * col_count
    nodes = tile_rows * row_count * tile_cols * col_count
    mr = tile_rows // CELL
    er = mr + 2 * HC
    tiles = tile_cols // LANES
    vmem = pl.BlockSpec(memory_space=pltpu.VMEM)
    smem = pl.BlockSpec(memory_space=pltpu.SMEM)
    params = pltpu.CompilerParams(vmem_limit_bytes=32 * 1024 * 1024)
    field = initial_field[0]
    sources = (field, information, kappa_squared, lumped_mass)
    rows_shape = jax.ShapeDtypeStruct((4 * HALO + SUB, tile_cols), F32)
    cols_shape = jax.ShapeDtypeStruct((4 * tile_rows * HALO // LANES + SUB, LANES), F32)
    up, down, left, right = pl.pallas_call(
        pack_kernel,
        in_specs=[smem] + [vmem] * 4,
        out_specs=[vmem] * 4,
        out_shape=[rows_shape, rows_shape, cols_shape, cols_shape],
        compiler_params=params,
        name="pack",
    )(noise_seeds, *sources)
    from_right = lax.ppermute(left, "col", ring(col_count, -1))
    from_left = lax.ppermute(right, "col", ring(col_count, 1))
    from_below = lax.ppermute(up, "row", ring(row_count, -1))
    from_above = lax.ppermute(down, "row", ring(row_count, 1))
    corner_shape = jax.ShapeDtypeStruct((6 * SUB, LANES), F32)
    corner_up, corner_down = pl.pallas_call(
        corner_kernel,
        in_specs=[vmem] * 2,
        out_specs=[vmem] * 2,
        out_shape=[corner_shape, corner_shape],
        compiler_params=params,
        name="corners",
    )(from_right, from_left)
    corner_below = lax.ppermute(corner_up, "row", ring(row_count, -1))
    corner_above = lax.ppermute(corner_down, "row", ring(row_count, 1))
    planes = CELL * CELL
    result, energy = pl.pallas_call(
        functools.partial(main_kernel, tile_rows, tile_cols, nodes),
        in_specs=[smem, smem] + [vmem] * 10,
        out_specs=[vmem] * 2,
        out_shape=[
            jax.ShapeDtypeStruct((tile_rows, tile_cols), F32),
            jax.ShapeDtypeStruct((devices, LANES), F32),
        ],
        scratch_shapes=[
            pltpu.VMEM((4 * (tiles + 1), tile_rows + 2 * HALO, LANES), F32),
            pltpu.VMEM((planes, er, 2 * LANES), F32),
            pltpu.VMEM((planes, er, 2 * LANES), F32),
            pltpu.VMEM((planes, er, 2 * LANES), F32),
            pltpu.VMEM((planes, er, 2 * LANES), F32),
            pltpu.VMEM((planes, er, 2 * LANES), F32),
            pltpu.VMEM((COLOURS * 10, er, 2 * LANES), F32),
            pltpu.VMEM((PHASES * 4, er, 2 * LANES), F32),
            pltpu.VMEM((PHASES + 1, SUB, LANES), F32),
            pltpu.VMEM((PHASES, 2, SUB, LANES), I32),
        ],
        compiler_params=params,
        name="sweeps",
    )(
        colour_order, noise_seeds, *sources,
        from_below, from_above, from_right, from_left, corner_below, corner_above,
    )
    shared = lax.all_to_all(energy, AXES, 0, 0, tiled=True)
    energies = jnp.sum(shared, axis=0)[:PHASES].reshape(SWEEPS, COLOURS, chains)
    return (result[None], energies)


def solution(mesh):
    placed = (
        P(None, "row", "col"),
        P("row", "col"),
        P("row", "col"),
        P("row", "col"),
        P("row", "col", None, None, None),
        P(),
    )
    return jax.shard_map(
        local, mesh=mesh, in_specs=placed, out_specs=(P(None, "row", "col"), P()), check_vma=False
    )
```

```python
import functools

import jax
import jax.numpy as jnp
from jax import lax
from jax.experimental import pallas as pl
from jax.experimental.pallas import tpu as pltpu
from jax.sharding import PartitionSpec as P

SWEEPS = 2
COLOURS = 4
PHASES = SWEEPS * COLOURS
HALO = 2 * PHASES
CELL = 4
HC = HALO // CELL
LANES = 128
SUB = 8
GROUP = LANES // CELL
AXES = ("row", "col")
F32 = jnp.float32
I32 = jnp.int32

unit_step = 1.0 / 8388608.0
mix_factor = 73244475
SEED_BASE = 32768

SIN_COEFFS = (
    6.283185306485777,
    -41.34170192921984,
    81.60520938153618,
    -76.70366601553475,
    41.99996083008805,
    -14.336855962945094,
)


def lane_iota(shape):
    return lax.broadcasted_iota(I32, shape, len(shape) - 1)


def sub_iota(shape):
    return lax.broadcasted_iota(I32, shape, len(shape) - 2)


def lane_gather(value, index):
    return jnp.take_along_axis(value, index, axis=1, mode="promise_in_bounds")


def lroll(value, amount):
    amount = amount % value.shape[1]
    return pltpu.roll(value, amount, 1) if amount else value


def pack_kernel(seeds_ref, *refs):
    sources, (up_ref, down_ref, left_ref, right_ref) = refs[:4], refs[4:8]
    edges, seeds_buf, sems = refs[8:]
    rows, cols = sources[0].shape
    per = LANES // HALO
    lane = lane_iota((SUB, LANES))
    copies = []

    def copy(source, target):
        made = pltpu.make_async_copy(source, target, sems.at[len(copies)])
        made.start()
        copies.append(made)

    copy(seeds_ref, seeds_buf)
    for a, source in enumerate(sources):
        copy(source.at[:, pl.ds(0, LANES)], edges.at[2 * a])
        copy(source.at[:, pl.ds(cols - LANES, LANES)], edges.at[2 * a + 1])
    for a, source in enumerate(sources):
        copy(source.at[pl.ds(0, HALO)], up_ref.at[pl.ds(a * HALO, HALO)])
        copy(source.at[pl.ds(rows - HALO, HALO)], down_ref.at[pl.ds(a * HALO, HALO)])
    copies[0].wait()
    base = 4 * HALO
    for sweep in range(SWEEPS):
        seeds = seeds_buf[0, 0, sweep]
        high = (seeds // SEED_BASE).astype(F32)
        low = (seeds % SEED_BASE).astype(F32)
        for out in (up_ref, down_ref, left_ref, right_ref):
            out[base + sweep : base + sweep + 1, 0:COLOURS] = high
            out[base + SWEEPS + sweep : base + SWEEPS + sweep + 1, 0:COLOURS] = low
    for a in range(4):
        for edge, out in ((0, left_ref), (1, right_ref)):
            copies[1 + 2 * a + edge].wait()
            for v in range(rows // (SUB * per)):
                packed = jnp.zeros((SUB, LANES), F32)
                for q in range(per):
                    top = SUB * (v * per + q)
                    piece = edges[2 * a + edge, top : top + SUB, :]
                    piece = lroll(piece, HALO * q - (LANES - HALO if edge else 0))
                    packed = jnp.where(lane // HALO == q, piece, packed)
                out[a * HALO + SUB * v : a * HALO + SUB * (v + 1), :] = packed
    for made in copies[9:]:
        made.wait()


def corner_kernel(right_ref, left_ref, up_ref, down_ref):
    lane = lane_iota((SUB, LANES))
    for a in range(4):
        for out, top, shift in ((up_ref, 0, 0), (down_ref, HALO - SUB, 2 * HALO)):
            r = right_ref[a * HALO + top : a * HALO + top + SUB, :]
            l = left_ref[a * HALO + top : a * HALO + top + SUB, :]
            r = lroll(r, shift)
            l = lroll(l, shift + 2 * HALO)
            out[a * SUB : (a + 1) * SUB, :] = jnp.where(lane < 2 * HALO, r, l)
    for out in (up_ref, down_ref):
        out[4 * SUB : 5 * SUB, :] = right_ref[4 * HALO : 4 * HALO + SUB, :]
        out[5 * SUB : 6 * SUB, :] = left_ref[4 * HALO : 4 * HALO + SUB, :]


def scramble(hashed):
    sixteen = jnp.full_like(hashed, 16)
    hashed = hashed ^ lax.shift_right_logical(hashed, sixteen)
    hashed = hashed * mix_factor
    hashed = hashed ^ lax.shift_right_logical(hashed, sixteen)
    hashed = hashed * mix_factor
    return hashed ^ lax.shift_right_logical(hashed, sixteen)


def gaussian(first):
    nine = jnp.full_like(first, 9)
    one = lax.shift_right_logical(scramble(first), nine).astype(F32)
    two = lax.shift_right_logical(scramble(first + 1), nine).astype(F32)
    u1 = (one + 1.0) * unit_step
    v = 0.25 - jnp.abs(two * unit_step - 0.5)
    square = v * v
    poly = jnp.full_like(v, SIN_COEFFS[-1])
    for coeff in SIN_COEFFS[-2::-1]:
        poly = poly * square + coeff
    return jnp.sqrt(-2.0 * jnp.log(u1)) * (-(v * poly))


BASE = SUB


def whole_rows(er, shift=0):
    return pl.ds(BASE + shift, er)


def lane_shift(value, cols):
    if not cols:
        return value
    moved = pltpu.roll(value, (-cols) % LANES, 2)
    other = jnp.concatenate([moved[1:2], moved[0:1]], axis=0)
    edge = LANES - 1 if cols > 0 else 0
    return jnp.where(lane_iota(value.shape) == edge, other, moved)


def locate(r, c):
    return (r % CELL) * CELL + c % CELL, r // CELL, c // CELL


def fetch(ref, er, r, c):
    plane, rows, cols = locate(r, c)
    return lane_shift(ref[plane, :, whole_rows(er, rows), :], cols)


def neighbour_sum(ref, er, r, c):
    return (
        fetch(ref, er, r - 1, c)
        + fetch(ref, er, r + 1, c)
        + fetch(ref, er, r, c - 1)
        + fetch(ref, er, r, c + 1)
    )


def fold(value):
    value = value[0]
    count = value.shape[0]
    sub = sub_iota((SUB, LANES))
    total = jnp.where(sub >= HC, value[0:SUB], value[count - SUB : count])
    for top in range(SUB, count - SUB, SUB):
        total = total + value[top : top + SUB]
    return total


def block_nodes(colour):
    r0, c0 = 2 * (colour // 2), 2 * (colour % 2)
    return [(r0, c0), (r0, c0 + 1), (r0 + 1, c0), (r0 + 1, c0 + 1)]


def column_planes(pieces):
    wide = lane_iota(pieces[0].shape)
    group = wide // GROUP
    turned = [
        lane_gather(piece, CELL * (wide % GROUP) + (group + CELL - t) % CELL)
        for t, piece in enumerate(pieces)
    ]
    result = []
    for c in range(CELL):
        value = turned[(-c) % CELL]
        for g in range(1, CELL):
            value = jnp.where(group == g, turned[(g - c) % CELL], value)
        result.append(lroll(value, -GROUP * c))
    return result


def natural_columns(planes):
    wide = lane_iota(planes[0].shape)
    group = wide // GROUP
    turned = [lroll(plane, GROUP * c) for c, plane in enumerate(planes)]
    result = []
    for t in range(CELL):
        value = turned[(-t) % CELL]
        for g in range(1, CELL):
            value = jnp.where(group == g, turned[(g - t) % CELL], value)
        back = GROUP * ((wide % CELL + t) % CELL) + wide // CELL
        result.append(lane_gather(value, back))
    return result


def node_offsets(tile_cols, row_cell, col_cell):
    return 2 * CELL * tile_cols * row_cell + 2 * CELL * col_cell


def prepare_kernel(
    tile_rows, tile_cols,
    order_ref, seeds_ref, x_ref, b_ref, kappa_ref, mass_ref, after_ref,
    X, B, S, I, Z,
    nat, sems,
):
    del after_ref
    mr = tile_rows // CELL
    tiles = tile_cols // LANES
    copies = []
    for a, source in enumerate((x_ref, b_ref, kappa_ref, mass_ref)):
        for t in range(tiles):
            made = pltpu.make_async_copy(
                source.at[:, pl.ds(t * LANES, LANES)], nat.at[a * tiles + t], sems.at[a * tiles + t]
            )
            made.start()
            copies.append(made)
    rows = pl.ds(BASE + HC, mr)
    offset_main = node_offsets(tile_cols, sub_iota((mr, LANES)), lane_iota((mr, LANES)))

    def noise_phase(phase, carry):
        colour = order_ref[phase % COLOURS]
        r0, c0 = 2 * (colour // 2), 2 * (colour % 2)
        own = seeds_ref[0, 0, phase // COLOURS, 0, phase % COLOURS]
        for n in range(4):
            extra = 2 * ((r0 + n // 2) * tile_cols + c0 + n % 2)
            Z[phase * 4 + n, 0, rows, :] = gaussian(offset_main + (own + extra))
        return carry

    lax.fori_loop(0, PHASES, noise_phase, 0)

    for made in copies:
        made.wait()

    def planes(a, r):
        return column_planes(
            [nat[a * tiles + t, pl.ds(r, mr, stride=CELL), :] for t in range(tiles)]
        )

    for r in range(CELL):
        for c, value in enumerate(planes(0, r)):
            X[r * CELL + c, 0, rows, :] = value
        for c, value in enumerate(planes(1, r)):
            B[r * CELL + c, 0, rows, :] = value
        for c, (kappa, mass) in enumerate(zip(planes(2, r), planes(3, r))):
            S[r * CELL + c, 0, rows, :] = kappa * mass + 4.0
            I[r * CELL + c, 0, rows, :] = 1.0 / mass


def sweep_kernel(
    tile_rows, tile_cols, nodes,
    order_ref, x_in, b_in, s_in, i_in, z_in,
    below_ref, above_ref, right_ref, left_ref, cbelow_ref, cabove_ref,
    out_ref, energy_ref, X, B, S, I, Z,
    nat, strip, W, LM, EN, ST,
):
    del x_in, b_in, s_in, i_in, z_in
    mr = tile_rows // CELL
    er = mr + 2 * HC
    tiles = tile_cols // LANES
    lane = lane_iota((SUB, LANES))
    sub = sub_iota((SUB, LANES))
    per = LANES // HALO
    every = whole_rows(er)
    top_rows, low_rows = pl.ds(BASE, HC), pl.ds(BASE + HC + mr, HC)

    for a in range(4):
        for t in range(tiles):
            lanes = slice(t * LANES, (t + 1) * LANES)
            for start, source in ((0, above_ref), (HALO, below_ref)):
                strip[a * tiles + t, start : start + HALO, :] = source[
                    a * HALO : (a + 1) * HALO, lanes
                ]

        def put(top, right, left):
            nat[a, top : top + SUB, :] = jnp.where(
                lane < HALO, right, jnp.where(lane >= LANES - HALO, left, 1.0)
            )

        for g in range(tile_rows // SUB):
            v, q = g // per, g % per
            rows = slice(a * HALO + SUB * v, a * HALO + SUB * (v + 1))
            put(
                HALO + SUB * g,
                lroll(right_ref[rows, :], -HALO * q),
                lroll(left_ref[rows, :], LANES - HALO - HALO * q),
            )
        for start, corner in ((0, cabove_ref), (HALO + tile_rows, cbelow_ref)):
            value = corner[a * SUB : (a + 1) * SUB, :]
            for h in range(HALO // SUB):
                put(
                    start + SUB * h,
                    lroll(value, -HALO * h),
                    lroll(value, LANES - HALO - 2 * HALO - HALO * h),
                )

    wide = lane_iota((er, LANES))
    halo_index = [CELL * (wide % GROUP) + c for c in range(CELL)]

    def strip_planes(a, r):
        return column_planes(
            [strip[a * tiles + t, pl.ds(r, SUB, stride=CELL), :] for t in range(tiles)]
        )

    def side_planes(a, r):
        outer = nat[a, pl.ds(r, er, stride=CELL), :]
        return [lane_gather(outer, halo_index[c]) for c in range(CELL)]

    def put_strip(ref, plane, value):
        ref[plane, 0, top_rows, :] = value[0:HC]
        ref[plane, 0, low_rows, :] = value[HC:SUB]

    for r in range(CELL):
        for a, ref in ((0, X), (1, B)):
            for c, value in enumerate(strip_planes(a, r)):
                put_strip(ref, r * CELL + c, value)
            for c, value in enumerate(side_planes(a, r)):
                ref[r * CELL + c, 1, every, :] = value
        for c, (kappa, mass) in enumerate(zip(strip_planes(2, r), strip_planes(3, r))):
            put_strip(S, r * CELL + c, kappa * mass + 4.0)
            put_strip(I, r * CELL + c, 1.0 / mass)
        for c, (kappa, mass) in enumerate(zip(side_planes(2, r), side_planes(3, r))):
            S[r * CELL + c, 1, every, :] = kappa * mass + 4.0
            I[r * CELL + c, 1, every, :] = 1.0 / mass

    energy = jnp.zeros((SUB, LANES), F32)
    for r in range(CELL):
        for c in range(CELL):
            plane = r * CELL + c
            field = X[plane, :, every, :]
            first = S[plane, :, every, :] * field - neighbour_sum(X, er, r, c)
            scaled = I[plane, :, every, :] * first
            W[plane, :, every, :] = scaled
            energy = energy + fold(0.5 * scaled * first - B[plane, :, every, :] * field)
    EN[0] = energy

    for colour in range(COLOURS):
        nodes_here = block_nodes(colour)
        inv = [I[r * CELL + c, :, every, :] for r, c in nodes_here]
        stiff = [S[r * CELL + c, :, every, :] for r, c in nodes_here]
        scaled = [stiff[n] * inv[n] for n in range(4)]
        diag = [stiff[n] * scaled[n] + neighbour_sum(I, er, *nodes_here[n]) for n in range(4)]
        m01, m02 = -(scaled[0] + scaled[1]), -(scaled[0] + scaled[2])
        m13, m23 = -(scaled[1] + scaled[3]), -(scaled[2] + scaled[3])
        m03, m12 = inv[1] + inv[2], inv[0] + inv[3]
        r0 = lax.rsqrt(diag[0])
        l10, l20, l30 = m01 * r0, m02 * r0, m03 * r0
        r1 = lax.rsqrt(diag[1] - l10 * l10)
        l21, l31 = (m12 - l20 * l10) * r1, (m13 - l30 * l10) * r1
        r2 = lax.rsqrt(diag[2] - l20 * l20 - l21 * l21)
        l32 = (m23 - l30 * l20 - l31 * l21) * r2
        r3 = lax.rsqrt(diag[3] - l30 * l30 - l31 * l31 - l32 * l32)
        for n, value in enumerate((r0, r1, r2, r3, l10, l20, l30, l21, l31, l32)):
            LM[colour * 10 + n] = value

    def whole(ref, top):
        tile = ref[top : top + SUB, 0:LANES].astype(I32)
        return tile[0:SWEEPS] * SEED_BASE + tile[SWEEPS : 2 * SWEEPS]

    base = 4 * HALO
    around = {
        "B": whole(below_ref, base), "T": whole(above_ref, base),
        "R": whole(right_ref, base), "L": whole(left_ref, base),
        "BR": whole(cbelow_ref, 4 * SUB), "BL": whole(cbelow_ref, 5 * SUB),
        "TR": whole(cabove_ref, 4 * SUB), "TL": whole(cabove_ref, 5 * SUB),
    }
    spot = lane % GROUP
    high = sub < HC
    in_right_corner = (lane >= 2 * HC) & (lane < 3 * HC)
    in_left_corner = (lane >= HC) & (lane < 2 * HC)
    in_corner = in_right_corner | in_left_corner
    for phase in range(PHASES):
        sweep, k = phase // COLOURS, phase % COLOURS
        pick = {
            key: jnp.broadcast_to(value[sweep : sweep + 1, k : k + 1], (SUB, LANES))
            for key, value in around.items()
        }
        ST[phase, 0] = jnp.where(high, pick["T"], pick["B"])
        side = jnp.where(spot < GROUP // 2, pick["R"], pick["L"])
        side = jnp.where(in_right_corner, jnp.where(high, pick["TR"], pick["BR"]), side)
        ST[phase, 1] = jnp.where(in_left_corner, jnp.where(high, pick["TL"], pick["BL"]), side)

    strip_cell = jnp.where(high, sub + mr - HC, sub - HC)
    offset_strip = node_offsets(tile_cols, strip_cell, lane)
    is_right = spot < GROUP // 2
    side_row = SUB * jnp.where(is_right, lane // GROUP, (lane // GROUP + 1) % CELL) + sub
    side_row = jnp.where(in_corner, strip_cell, side_row)
    side_col = jnp.where(is_right, spot, spot + LANES - GROUP)
    side_col = jnp.where(in_right_corner, lane - 2 * HC, side_col)
    side_col = jnp.where(in_left_corner, lane + LANES - 2 * HC, side_col)
    offset_side = node_offsets(tile_cols, side_row, side_col)

    def noise_phase(phase, carry):
        colour = order_ref[phase % COLOURS]
        r0, c0 = 2 * (colour // 2), 2 * (colour % 2)
        strip_seed = ST[phase, 0]
        side_seed = ST[phase, 1]
        for n in range(4):
            extra = 2 * ((r0 + n // 2) * tile_cols + c0 + n % 2)
            at = phase * 4 + n
            value = gaussian(offset_strip + strip_seed + extra)
            put_strip(Z, at, value)
            side = gaussian(offset_side + side_seed + extra)
            for g in range(mr // SUB):
                Z[at, 1, pl.ds(BASE + HC + SUB * g, SUB), :] = lroll(side, -GROUP * g)
            value = lroll(side, -2 * HC)
            Z[at, 1, top_rows, :] = value[0:HC]
            Z[at, 1, low_rows, :] = value[HC:SUB]
        return carry

    lax.fori_loop(0, PHASES, noise_phase, 0)

    def phase_body(colour, phase):
        nodes_here = block_nodes(colour)
        r0, c0 = nodes_here[0]
        own = [r * CELL + c for r, c in nodes_here]
        w = {}
        for r in range(r0 - 1, r0 + 3):
            for c in range(c0 - 1, c0 + 3):
                inside_row, inside_col = r0 <= r <= r0 + 1, c0 <= c <= c0 + 1
                if inside_row or inside_col:
                    w[r, c] = fetch(W, er, r, c)
        stiff = [S[plane, :, every, :] for plane in own]
        residual = []
        for n, (r, c) in enumerate(nodes_here):
            around_sum = w[r - 1, c] + w[r + 1, c] + w[r, c - 1] + w[r, c + 1]
            residual.append(B[own[n], :, every, :] - (stiff[n] * w[r, c] - around_sum))
        q0, q1, q2, q3, l10, l20, l30, l21, l31, l32 = [LM[colour * 10 + n] for n in range(10)]
        z = [Z[phase * 4 + n, :, every, :] for n in range(4)]
        f0 = residual[0] * q0
        f1 = (residual[1] - l10 * f0) * q1
        f2 = (residual[2] - l20 * f0 - l21 * f1) * q2
        f3 = (residual[3] - l30 * f0 - l31 * f1 - l32 * f2) * q3
        y0, y1, y2, y3 = f0 + z[0], f1 + z[1], f2 + z[2], f3 + z[3]
        d3 = y3 * q3
        d2 = (y2 - l32 * d3) * q2
        d1 = (y1 - l21 * d2 - l31 * d3) * q1
        d0 = (y0 - l10 * d1 - l20 * d2 - l30 * d3) * q0
        change = jnp.zeros((SUB, LANES), F32)
        for n, f in enumerate((f0, f1, f2, f3)):
            change = change + fold(z[n] * z[n] - f * f)
        EN[phase + 1] = 0.5 * change
        delta = [d0, d1, d2, d3]
        for n in range(4):
            X[own[n], :, every, :] = X[own[n], :, every, :] + delta[n]
        for n, (across, down) in enumerate(((1, 2), (0, 3), (3, 0), (2, 1))):
            step = stiff[n] * delta[n] - (delta[across] + delta[down])
            W[own[n], :, every, :] = w[nodes_here[n]] + I[own[n], :, every, :] * step
        for n, (r, c) in enumerate(nodes_here):
            for rr, cc in ((r - 1 if r == r0 else r + 1, c), (r, c - 1 if c == c0 else c + 1)):
                plane, rows, cols = locate(rr, cc)
                at = whole_rows(er, rows)
                W[plane, :, at, :] = W[plane, :, at, :] - I[plane, :, at, :] * lane_shift(
                    delta[n], -cols
                )

    def run_phase(phase, carry):
        colour = order_ref[phase % COLOURS]
        for option in range(COLOURS):
            @pl.when(colour == option)
            def _():
                phase_body(option, phase)
        return carry

    lax.fori_loop(0, PHASES, run_phase, 0)

    running = EN[0]
    result = jnp.zeros((1, LANES), F32)
    first_row = lane_iota((1, LANES))
    for phase in range(PHASES):
        if phase:
            running = running + EN[phase]
        total = jnp.sum(jnp.sum(running, axis=0, keepdims=True), axis=1, keepdims=True)
        result = jnp.where(first_row == phase, total, result)
    energy_ref[...] = jnp.broadcast_to(result / nodes, energy_ref.shape)

    inside = pl.ds(BASE + HC, mr)
    for r in range(CELL):
        columns = natural_columns([X[r * CELL + c, 0, inside, :] for c in range(CELL)])
        for t, value in enumerate(columns):
            nat[t, pl.ds(r, mr, stride=CELL), :] = value
    for t in range(tiles):
        out_ref[:, t * LANES : (t + 1) * LANES] = nat[t, 0:tile_rows, :]


def ring(count, step):
    return [(i, (i + step) % count) for i in range(count)]


def local(initial_field, information, kappa_squared, lumped_mass, noise_seeds, colour_order):
    chains, tile_rows, tile_cols = initial_field.shape
    row_count, col_count = lax.axis_size("row"), lax.axis_size("col")
    devices = row_count * col_count
    nodes = tile_rows * row_count * tile_cols * col_count
    mr = tile_rows // CELL
    er = mr + 2 * HC
    tiles = tile_cols // LANES
    vmem = pl.BlockSpec(memory_space=pltpu.VMEM)
    smem = pl.BlockSpec(memory_space=pltpu.SMEM)
    hbm = pl.BlockSpec(memory_space=pltpu.HBM)
    params = pltpu.CompilerParams(vmem_limit_bytes=16 * 1024 * 1024)
    field = initial_field[0]
    seeds = jnp.swapaxes(noise_seeds, 3, 4)
    sources = [
        pltpu.with_memory_space_constraint(value, pltpu.HBM)
        for value in (field, information, kappa_squared, lumped_mass)
    ]
    rows_shape = jax.ShapeDtypeStruct((4 * HALO + SUB, tile_cols), F32)
    cols_shape = jax.ShapeDtypeStruct((4 * tile_rows * HALO // LANES + SUB, LANES), F32)
    up, down, left, right = pl.pallas_call(
        pack_kernel,
        in_specs=[hbm] * 5,
        out_specs=[vmem] * 4,
        out_shape=[rows_shape, rows_shape, cols_shape, cols_shape],
        scratch_shapes=[
            pltpu.VMEM((8, tile_rows, LANES), F32),
            pltpu.VMEM(seeds.shape, I32),
            pltpu.SemaphoreType.DMA((17,)),
        ],
        compiler_params=params,
        name="pack",
    )(pltpu.with_memory_space_constraint(seeds, pltpu.HBM), *sources)
    from_right = lax.ppermute(left, "col", ring(col_count, -1))
    from_left = lax.ppermute(right, "col", ring(col_count, 1))
    from_below = lax.ppermute(up, "row", ring(row_count, -1))
    from_above = lax.ppermute(down, "row", ring(row_count, 1))
    corner_shape = jax.ShapeDtypeStruct((6 * SUB, LANES), F32)
    corner_up, corner_down = pl.pallas_call(
        corner_kernel,
        in_specs=[vmem] * 2,
        out_specs=[vmem] * 2,
        out_shape=[corner_shape, corner_shape],
        compiler_params=params,
        name="corners",
    )(from_right, from_left)
    corner_below = lax.ppermute(corner_up, "row", ring(row_count, -1))
    corner_above = lax.ppermute(corner_down, "row", ring(row_count, 1))
    planes = CELL * CELL
    plane_shape = jax.ShapeDtypeStruct((planes, 2, er + 2 * BASE, LANES), F32)
    noise_shape = jax.ShapeDtypeStruct((PHASES * 4, 2, er + 2 * BASE, LANES), F32)
    prepared = pl.pallas_call(
        functools.partial(prepare_kernel, tile_rows, tile_cols),
        in_specs=[smem, smem] + [hbm] * 4 + [vmem],
        out_specs=[vmem] * 5,
        out_shape=[plane_shape] * 4 + [noise_shape],
        scratch_shapes=[
            pltpu.VMEM((4 * tiles, tile_rows, LANES), F32),
            pltpu.SemaphoreType.DMA((4 * tiles,)),
        ],
        compiler_params=params,
        cost_estimate=pl.CostEstimate(flops=20_000_000, bytes_accessed=1_000_000, transcendentals=0),
        name="prepare",
    )(colour_order, seeds, *sources, corner_up)
    result, energy, *_ = pl.pallas_call(
        functools.partial(sweep_kernel, tile_rows, tile_cols, nodes),
        in_specs=[smem] + [vmem] * 11,
        out_specs=[vmem] * 7,
        out_shape=[
            jax.ShapeDtypeStruct((tile_rows, tile_cols), F32),
            jax.ShapeDtypeStruct((devices, LANES), F32),
        ]
        + [plane_shape] * 4
        + [noise_shape],
        input_output_aliases={1: 2, 2: 3, 3: 4, 4: 5, 5: 6},
        scratch_shapes=[
            pltpu.VMEM((max(4, tiles), tile_rows + 2 * HALO, LANES), F32),
            pltpu.VMEM((4 * tiles, 2 * HALO, LANES), F32),
            pltpu.VMEM((planes, 2, er + 2 * BASE, LANES), F32),
            pltpu.VMEM((COLOURS * 10, 2, er, LANES), F32),
            pltpu.VMEM((PHASES + 1, SUB, LANES), F32),
            pltpu.VMEM((PHASES, 2, SUB, LANES), I32),
        ],
        compiler_params=params,
        name="sweeps",
    )(
        colour_order, *prepared,
        from_below, from_above, from_right, from_left, corner_below, corner_above,
    )
    shared = lax.all_to_all(energy, AXES, 0, 0, tiled=True)
    energies = jnp.sum(shared, axis=0)[:PHASES].reshape(SWEEPS, COLOURS, chains)
    return (result[None], energies)


def solution(mesh):
    placed = (
        P(None, "row", "col"),
        P("row", "col"),
        P("row", "col"),
        P("row", "col"),
        P("row", "col", None, None, None),
        P(),
    )
    return jax.shard_map(
        local, mesh=mesh, in_specs=placed, out_specs=(P(None, "row", "col"), P()), check_vma=False
    )
```

```python
import functools

import jax
import jax.numpy as jnp
from jax import lax
from jax.experimental import pallas as pl
from jax.experimental.pallas import tpu as pltpu
from jax.sharding import PartitionSpec as P

SWEEPS = 2
COLOURS = 4
PHASES = SWEEPS * COLOURS
HALO = 2 * PHASES
CELL = 4
HC = HALO // CELL
LANES = 128
SUB = 8
GROUP = LANES // CELL
AXES = ("row", "col")
F32 = jnp.float32
I32 = jnp.int32

unit_step = 1.0 / 8388608.0
mix_factor = 73244475
SEED_BASE = 32768

SIN_COEFFS = (
    6.283185306485777,
    -41.34170192921984,
    81.60520938153618,
    -76.70366601553475,
    41.99996083008805,
    -14.336855962945094,
)


def lane_iota(shape):
    return lax.broadcasted_iota(I32, shape, len(shape) - 1)


def sub_iota(shape):
    return lax.broadcasted_iota(I32, shape, len(shape) - 2)


def lane_gather(value, index):
    return jnp.take_along_axis(value, index, axis=1, mode="promise_in_bounds")


def lroll(value, amount):
    amount = amount % value.shape[1]
    return pltpu.roll(value, amount, 1) if amount else value


SLOT = 8


def slot_gather(value, left):
    wide = lane_iota(value.shape)
    at = (wide + SLOT // 2) % LANES if left else wide
    index = CELL * (at % CELL) + (at % GROUP) // SLOT
    return lane_gather(value, index + (LANES - HALO if left else 0))


def lane_group(left):
    lane = lane_iota((SUB, LANES))
    return ((lane + SLOT // 2) % LANES if left else lane) // GROUP


def pick_group(group, values):
    result = values[0]
    for g in range(1, CELL):
        result = jnp.where(group == g, values[g], result)
    return result


def join_sides(right, left):
    return jnp.where(lane_iota(right.shape) % SLOT < SLOT // 2, right, left)


def pack_kernel(seeds_ref, *refs):
    sources, (up_ref, down_ref, left_ref, right_ref) = refs[:4], refs[4:8]
    edges, seeds_buf, sems = refs[8:]
    rows, cols = sources[0].shape
    mr = rows // CELL
    copies = []

    def copy(source, target):
        made = pltpu.make_async_copy(source, target, sems.at[len(copies)])
        made.start()
        copies.append(made)

    copy(seeds_ref, seeds_buf)
    for a, source in enumerate(sources):
        copy(source.at[:, pl.ds(0, LANES)], edges.at[2 * a])
        copy(source.at[:, pl.ds(cols - LANES, LANES)], edges.at[2 * a + 1])
    for a, source in enumerate(sources):
        copy(source.at[pl.ds(0, HALO)], up_ref.at[pl.ds(a * HALO, HALO)])
        copy(source.at[pl.ds(rows - HALO, HALO)], down_ref.at[pl.ds(a * HALO, HALO)])
    for made in copies:
        made.wait()
    for sweep in range(SWEEPS):
        seeds = seeds_buf[0, 0, sweep]
        high = (seeds // SEED_BASE).astype(F32)
        low = (seeds % SEED_BASE).astype(F32)
        for out in (up_ref, down_ref, left_ref, right_ref):
            base = out.shape[0] - SUB
            out[base + sweep : base + sweep + 1, 0:COLOURS] = high
            out[base + SWEEPS + sweep : base + SWEEPS + sweep + 1, 0:COLOURS] = low

    def pack(a, carry):
        for edge, out in ((0, left_ref), (1, right_ref)):
            group = lane_group(edge == 1)
            for r in range(CELL):
                value = slot_gather(edges[2 * a + edge, pl.ds(r, mr, stride=CELL), :], edge == 1)
                parts = [value[SUB * g : SUB * (g + 1)] for g in range(CELL)]
                at = pl.multiple_of((a * CELL + r) * SUB, SUB)
                out[pl.ds(at, SUB), :] = pick_group(group, parts)
        return carry

    lax.fori_loop(0, 4, pack, 0)


def corner_kernel(right_ref, left_ref, up_ref, down_ref):
    group = lane_group(True)
    for a in range(4):
        sides = []
        for r in range(CELL):
            rows = slice((a * CELL + r) * SUB, (a * CELL + r + 1) * SUB)
            sides.append(join_sides(right_ref[rows, :], left_ref[rows, :]))
        rows = slice(a * SUB, (a + 1) * SUB)
        up_ref[rows, :] = pick_group(group, [lroll(v, GROUP * r) for r, v in enumerate(sides)])
        down_ref[rows, :] = pick_group(
            group, [lroll(v, GROUP * (r + 1)) for r, v in enumerate(sides)]
        )
    base = right_ref.shape[0] - SUB
    for out in (up_ref, down_ref):
        out[4 * SUB : 5 * SUB, :] = right_ref[base : base + SUB, :]
        out[5 * SUB : 6 * SUB, :] = left_ref[base : base + SUB, :]


def scramble(hashed):
    sixteen = jnp.full_like(hashed, 16)
    hashed = hashed ^ lax.shift_right_logical(hashed, sixteen)
    hashed = hashed * mix_factor
    hashed = hashed ^ lax.shift_right_logical(hashed, sixteen)
    hashed = hashed * mix_factor
    return hashed ^ lax.shift_right_logical(hashed, sixteen)


def gaussian(first):
    nine = jnp.full_like(first, 9)
    one = lax.shift_right_logical(scramble(first), nine).astype(F32)
    two = lax.shift_right_logical(scramble(first + 1), nine).astype(F32)
    u1 = (one + 1.0) * unit_step
    v = 0.25 - jnp.abs(two * unit_step - 0.5)
    square = v * v
    poly = jnp.full_like(v, SIN_COEFFS[-1])
    for coeff in SIN_COEFFS[-2::-1]:
        poly = poly * square + coeff
    square = -2.0 * jnp.log(u1)
    return square * lax.rsqrt(jnp.maximum(square, 1e-30)) * (-(v * poly))


BASE = SUB


def rows_at(first, count):
    return pl.ds(BASE + first, count)


def lane_shift(value, amount, edge):
    moved = pltpu.roll(value, amount, 2)
    other = jnp.concatenate([moved[1:2], moved[0:1]], axis=0)
    return jnp.where(lane_iota(value.shape) == edge, other, moved)


def fold(value):
    count = value.shape[0]
    sub = sub_iota((SUB, LANES))
    total = jnp.where(sub >= HC, value[0:SUB], value[count - SUB : count])
    for top in range(SUB, count - SUB, SUB):
        total = total + value[top : top + SUB]
    return total


def gather_cells(value):
    wide = lane_iota(value.shape)
    return lane_gather(value, CELL * (wide % GROUP) + wide // GROUP)


def scatter_cells(value):
    wide = lane_iota(value.shape)
    return lane_gather(value, GROUP * (wide % CELL) + wide // CELL)


def column_planes(pieces):
    group = lane_iota(pieces[0].shape) // GROUP
    turned = [lroll(gather_cells(piece), GROUP * t) for t, piece in enumerate(pieces)]
    return [
        lroll(pick_group(group, [turned[(g - c) % CELL] for g in range(CELL)]), -GROUP * c)
        for c in range(CELL)
    ]


def natural_columns(planes):
    group = lane_iota(planes[0].shape) // GROUP
    turned = [lroll(plane, GROUP * c) for c, plane in enumerate(planes)]
    return [
        scatter_cells(
            lroll(pick_group(group, [turned[(g - t) % CELL] for g in range(CELL)]), -GROUP * t)
        )
        for t in range(CELL)
    ]


def put_ends(ref, plane, half, value):
    count = ref.shape[2] - 2 * BASE
    ref[plane, half, pl.ds(BASE + count - HC, HC), :] = value[0:HC]
    ref[plane, half, pl.ds(BASE, HC), :] = value[HC:SUB]


def node_offsets(tile_cols, row_cell, col_cell):
    return 2 * CELL * tile_cols * row_cell + 2 * CELL * col_cell


def phase_extra(colour, n, tile_cols):
    row, col = 2 * (colour // 2) + n // 2, 2 * (colour % 2) + n % 2
    return 2 * (row * tile_cols + col)


def noise_kernel(
    tile_rows, tile_cols,
    order_ref, seeds_ref, x_ref, b_ref, kappa_ref, mass_ref,
    Z, nat,
    order, seeds, sems,
):
    mr = tile_rows // CELL
    tiles = tile_cols // LANES
    copies = []

    def copy(source, target):
        made = pltpu.make_async_copy(source, target, sems.at[len(copies)])
        made.start()
        copies.append(made)

    copy(order_ref, order)
    copy(seeds_ref, seeds)
    for a, source in enumerate((x_ref, b_ref, kappa_ref, mass_ref)):
        for t in range(tiles):
            copy(
                source.at[:, pl.ds(t * LANES, LANES)],
                nat.at[a * tiles + t, pl.ds(0, tile_rows)],
            )
    copies[0].wait()
    copies[1].wait()
    offset_main = node_offsets(tile_cols, sub_iota((mr, LANES)), lane_iota((mr, LANES)))

    def noise_phase(phase, carry):
        own = seeds[0, 0, phase // COLOURS, 0, phase % COLOURS]
        colour = order[phase % COLOURS]
        for n in range(4):
            start = own + phase_extra(colour, n, tile_cols)
            Z[phase * 4 + n, 0, rows_at(HC, mr), :] = gaussian(offset_main + start)
        return carry

    lax.fori_loop(0, PHASES, noise_phase, 0)
    for made in copies[2:]:
        made.wait()


def planes_kernel(
    tile_rows, tile_cols,
    nat_in, below_ref, above_ref, right_ref, left_ref,
    X, B, S, I, nat,
):
    del nat_in
    mr = tile_rows // CELL
    er = mr + 2 * HC
    tiles = tile_cols // LANES

    def strips(a, carry):
        for t in range(tiles):
            lanes = slice(t * LANES, (t + 1) * LANES)
            at = pl.ds(pl.multiple_of(a * HALO, HALO), HALO)
            for start, source in ((0, below_ref), (HALO, above_ref)):
                nat[a * tiles + t, pl.ds(tile_rows + start, HALO), :] = source[at, lanes]
        return carry

    lax.fori_loop(0, 4, strips, 0)

    def put(ref, plane, value):
        ref[plane, 0, rows_at(HC, mr), :] = value[0:mr]
        put_ends(ref, plane, 0, value[mr:er])

    def row(r, carry):
        inner, outer = [], []
        for a in range(4):
            inner.append(
                column_planes(
                    [nat[a * tiles + t, pl.ds(r, er, stride=CELL), :] for t in range(tiles)]
                )
            )
            rows = pl.ds(pl.multiple_of((a * CELL + r) * SUB, SUB), SUB)
            side = join_sides(right_ref[rows, :], left_ref[rows, :])
            outer.append([lroll(side, -SLOT * slot) for slot in range(LANES // SLOT)])
        for c in range(CELL):
            plane = r * CELL + c
            put(X, plane, inner[0][c])
            put(B, plane, inner[1][c])
            put(S, plane, inner[2][c] * inner[3][c] + 4.0)
            put(I, plane, 1.0 / inner[3][c])
            for g in range(CELL):
                slot = CELL * g + c
                at = rows_at(HC + SUB * g, SUB)
                X[plane, 1, at, :] = outer[0][slot]
                B[plane, 1, at, :] = outer[1][slot]
                S[plane, 1, at, :] = outer[2][slot] * outer[3][slot] + 4.0
                I[plane, 1, at, :] = 1.0 / outer[3][slot]
        return carry

    lax.fori_loop(0, CELL, row, 0)


def sweep_kernel(
    tile_rows, tile_cols, nodes,
    order_ref, x_in, b_in, s_in, i_in, z_in,
    below_ref, above_ref, right_ref, left_ref, cbelow_ref, cabove_ref,
    out_ref, energy_ref, X, B, S, I, Z,
    W, D, EN, nat, order, around, sems,
):
    del x_in, b_in, s_in, i_in, z_in
    copies = []

    def copy(source, target):
        made = pltpu.make_async_copy(source, target, sems.at[len(copies)])
        made.start()
        copies.append(made)

    copy(order_ref, order)
    for at, (ref, back) in enumerate((
        (right_ref, 1), (left_ref, 1), (above_ref, 1), (below_ref, 1),
        (cabove_ref, 2), (cabove_ref, 1), (cbelow_ref, 2), (cbelow_ref, 1),
    )):
        top = ref.shape[0] - back * SUB
        copy(ref.at[pl.ds(top, SUB), pl.ds(0, LANES)], around.at[at])
    mr = tile_rows // CELL
    er = mr + 2 * HC
    tiles = tile_cols // LANES
    lane = lane_iota((SUB, LANES))
    sub = sub_iota((SUB, LANES))
    low = sub < HC

    corner = []
    for a in range(4):
        at = slice(a * SUB, (a + 1) * SUB)
        corner.append(jnp.where(low, cbelow_ref[at, :], cabove_ref[at, :]))

    def corners(r, carry):
        for c in range(CELL):
            plane = r * CELL + c
            value = [pltpu.roll(v, (2 * LANES - GROUP * r - SLOT * c) % LANES, 1) for v in carry]
            put_ends(X, plane, 1, value[0])
            put_ends(B, plane, 1, value[1])
            put_ends(S, plane, 1, value[2] * value[3] + 4.0)
            put_ends(I, plane, 1, 1.0 / value[3])
        return carry

    lax.fori_loop(0, CELL, corners, tuple(corner))

    every = rows_at(0, er)

    def start(r, energy):
        above, up = (r + CELL - 1) % CELL, jnp.where(r == 0, -1, 0)
        below, down = (r + 1) % CELL, jnp.where(r == CELL - 1, 1, 0)
        field = [X[r * CELL + c, :, every, :] for c in range(CELL)]
        inv = [I[r * CELL + c, :, every, :] for c in range(CELL)]

        def around_sum(ref, value, c):
            left = value[c - 1] if c else lane_shift(value[CELL - 1], 1, 0)
            right = value[c + 1] if c < CELL - 1 else lane_shift(value[0], LANES - 1, LANES - 1)
            return (
                ref[above * CELL + c, :, rows_at(up, er), :]
                + ref[below * CELL + c, :, rows_at(down, er), :]
                + left
                + right
            )

        for c in range(CELL):
            plane = r * CELL + c
            stiff = S[plane, :, every, :]
            first = stiff * field[c] - around_sum(X, field, c)
            scaled = inv[c] * first
            W[plane, :, every, :] = scaled
            D[plane, :, every, :] = stiff * stiff * inv[c] + around_sum(I, inv, c)
            part = 0.5 * scaled[0] * first[0] - B[plane, 0, every, :] * field[c][0]
            energy = energy + fold(part)
        return energy

    EN[0] = lax.fori_loop(0, CELL, start, jnp.zeros((SUB, LANES), F32))

    for made in copies:
        made.wait()
    spot = lane % GROUP
    is_right = spot < GROUP // 2
    in_right_corner = (lane >= 2 * HC) & (lane < 3 * HC)
    in_left_corner = (lane >= HC) & (lane < 2 * HC)
    end_cell = jnp.where(low, sub, sub + mr - 2 * HC)
    side_row = SUB * jnp.where(is_right, lane // GROUP, (lane // GROUP + 1) % CELL) + sub
    side_row = jnp.where(in_right_corner | in_left_corner, end_cell, side_row)
    side_col = jnp.where(is_right, spot, spot + LANES - GROUP)
    side_col = jnp.where(in_right_corner, lane - 2 * HC, side_col)
    side_col = jnp.where(in_left_corner, lane + LANES - 2 * HC, side_col)
    offset_side = node_offsets(tile_cols, side_row, side_col)
    offset_ends = node_offsets(tile_cols, end_cell, lane)

    def run_phase(phase, carry):
        sweep, k = phase // COLOURS, phase % COLOURS
        colour = order[k]
        ci, cj = colour // 2, colour % 2
        r0, c0 = 2 * ci, 2 * cj

        def seed(at):
            return around[at, sweep, k].astype(I32) * SEED_BASE + around[
                at, SWEEPS + sweep, k
            ].astype(I32)

        ends_seed = offset_ends + jnp.where(low, seed(3), seed(2))
        side_seed = jnp.where(is_right, seed(0), seed(1))
        side_seed = jnp.where(in_right_corner, jnp.where(low, seed(6), seed(4)), side_seed)
        side_seed = jnp.where(in_left_corner, jnp.where(low, seed(7), seed(5)), side_seed)
        side_seed = offset_side + side_seed
        for n in range(4):
            at = phase * 4 + n
            extra = phase_extra(colour, n, tile_cols)
            put_ends(Z, at, 0, gaussian(ends_seed + extra))
            value = gaussian(side_seed + extra)
            for g in range(mr // SUB):
                Z[at, 1, rows_at(HC + SUB * g, SUB), :] = lroll(value, -GROUP * g)
            put_ends(Z, at, 1, lroll(value, -2 * HC))
        z = [Z[phase * 4 + n, :, every, :] for n in range(4)]

        own = [(r0 + n // 2) * CELL + c0 + n % 2 for n in range(4)]
        above, up = (r0 + CELL - 1) % CELL, ci - 1
        below, down = (r0 + 2) % CELL, ci
        left, right = (c0 + CELL - 1) % CELL, (c0 + 2) % CELL
        above_rows, below_rows = rows_at(up, er), rows_at(down, er)
        w_own = [W[plane, :, every, :] for plane in own]
        w_above = [W[above * CELL + c0 + i, :, above_rows, :] for i in range(2)]
        w_below = [W[below * CELL + c0 + i, :, below_rows, :] for i in range(2)]
        w_left = [
            lane_shift(W[(r0 + i) * CELL + left, :, every, :], 1 - cj, -cj) for i in range(2)
        ]
        w_right = [
            lane_shift(
                W[(r0 + i) * CELL + right, :, every, :], (LANES - 1) * cj, LANES * cj - 1
            )
            for i in range(2)
        ]
        inv = [I[plane, :, every, :] for plane in own]
        stiff = [S[plane, :, every, :] for plane in own]
        sums = [
            w_above[0] + w_own[2] + w_left[0] + w_own[1],
            w_above[1] + w_own[3] + w_own[0] + w_right[0],
            w_own[0] + w_below[0] + w_left[1] + w_own[3],
            w_own[1] + w_below[1] + w_own[2] + w_right[1],
        ]
        residual = [
            B[own[n], :, every, :] - (stiff[n] * w_own[n] - sums[n]) for n in range(4)
        ]
        scaled = [stiff[n] * inv[n] for n in range(4)]
        diag = [D[plane, :, every, :] for plane in own]
        m01, m02 = -(scaled[0] + scaled[1]), -(scaled[0] + scaled[2])
        m13, m23 = -(scaled[1] + scaled[3]), -(scaled[2] + scaled[3])
        m03, m12 = inv[1] + inv[2], inv[0] + inv[3]
        q0 = lax.rsqrt(diag[0])
        l10, l20, l30 = m01 * q0, m02 * q0, m03 * q0
        q1 = lax.rsqrt(diag[1] - l10 * l10)
        l21, l31 = (m12 - l20 * l10) * q1, (m13 - l30 * l10) * q1
        q2 = lax.rsqrt(diag[2] - l20 * l20 - l21 * l21)
        l32 = (m23 - l30 * l20 - l31 * l21) * q2
        q3 = lax.rsqrt(diag[3] - l30 * l30 - l31 * l31 - l32 * l32)
        f0 = residual[0] * q0
        f1 = (residual[1] - l10 * f0) * q1
        f2 = (residual[2] - l20 * f0 - l21 * f1) * q2
        f3 = (residual[3] - l30 * f0 - l31 * f1 - l32 * f2) * q3
        y0, y1, y2, y3 = f0 + z[0], f1 + z[1], f2 + z[2], f3 + z[3]
        d3 = y3 * q3
        d2 = (y2 - l32 * d3) * q2
        d1 = (y1 - l21 * d2 - l31 * d3) * q1
        d0 = (y0 - l10 * d1 - l20 * d2 - l30 * d3) * q0
        delta = [d0, d1, d2, d3]
        for n in range(4):
            X[own[n], 0, every, :] = X[own[n], 0, every, :] + delta[n][0]
        change = 0.0
        for n, f in enumerate((f0, f1, f2, f3)):
            change = change + (z[n][0] * z[n][0] - f[0] * f[0])
        EN[phase + 1] = 0.5 * fold(change)
        for n, (across, beside) in enumerate(((1, 2), (0, 3), (3, 0), (2, 1))):
            step = stiff[n] * delta[n] - (delta[across] + delta[beside])
            W[own[n], :, every, :] = w_own[n] + inv[n] * step

        def spread(plane, rows, value):
            W[plane, :, rows, :] = W[plane, :, rows, :] - I[plane, :, rows, :] * value

        for i in range(2):
            spread(above * CELL + c0 + i, above_rows, delta[i])
            spread(below * CELL + c0 + i, below_rows, delta[2 + i])
            spread(
                (r0 + i) * CELL + left, every,
                lane_shift(delta[2 * i], (LANES - 1) * (1 - cj), LANES * (1 - cj) - 1),
            )
            spread(
                (r0 + i) * CELL + right, every, lane_shift(delta[2 * i + 1], cj, cj - 1)
            )
        return carry

    lax.fori_loop(0, PHASES, run_phase, 0)

    running = EN[0]
    result = jnp.zeros((1, LANES), F32)
    first_row = lane_iota((1, LANES))
    for phase in range(PHASES):
        if phase:
            running = running + EN[phase]
        total = jnp.sum(jnp.sum(running, axis=0, keepdims=True), axis=1, keepdims=True)
        result = jnp.where(first_row == phase, total, result)
    energy_ref[...] = jnp.broadcast_to(result / nodes, energy_ref.shape)

    def restore(i, carry):
        for r in (2 * i, 2 * i + 1):
            columns = natural_columns(
                [X[r * CELL + c, 0, rows_at(HC, mr), :] for c in range(CELL)]
            )
            for t, value in enumerate(columns):
                nat[t, pl.ds(r, mr, stride=CELL), :] = value
        return carry

    lax.fori_loop(0, CELL // 2, restore, 0)
    for t in range(tiles):
        out_ref[:, t * LANES : (t + 1) * LANES] = nat[t]


def ring(count, step):
    return [(i, (i + step) % count) for i in range(count)]


def estimate(flops):
    return pl.CostEstimate(flops=flops, bytes_accessed=1_000_000, transcendentals=0)


def local(initial_field, information, kappa_squared, lumped_mass, noise_seeds, colour_order):
    chains, tile_rows, tile_cols = initial_field.shape
    row_count, col_count = lax.axis_size("row"), lax.axis_size("col")
    devices = row_count * col_count
    nodes = tile_rows * row_count * tile_cols * col_count
    mr = tile_rows // CELL
    er = mr + 2 * HC
    tiles = tile_cols // LANES
    vmem = pl.BlockSpec(memory_space=pltpu.VMEM)
    hbm = pl.BlockSpec(memory_space=pltpu.HBM)
    params = pltpu.CompilerParams(vmem_limit_bytes=16 * 1024 * 1024)

    def in_hbm(value):
        return pltpu.with_memory_space_constraint(value, pltpu.HBM)

    seeds = in_hbm(jnp.swapaxes(noise_seeds, 3, 4))
    order = in_hbm(colour_order)
    sources = [
        in_hbm(value) for value in (initial_field[0], information, kappa_squared, lumped_mass)
    ]
    rows_shape = jax.ShapeDtypeStruct((4 * HALO + SUB, tile_cols), F32)
    cols_shape = jax.ShapeDtypeStruct((4 * CELL * SUB + SUB, LANES), F32)
    up, down, left, right = pl.pallas_call(
        pack_kernel,
        in_specs=[hbm] * 5,
        out_specs=[vmem] * 4,
        out_shape=[rows_shape, rows_shape, cols_shape, cols_shape],
        scratch_shapes=[
            pltpu.VMEM((8, tile_rows, LANES), F32),
            pltpu.VMEM(seeds.shape, I32),
            pltpu.SemaphoreType.DMA((17,)),
        ],
        compiler_params=params,
        name="pack",
    )(seeds, *sources)
    from_right = lax.ppermute(left, "col", ring(col_count, -1))
    from_left = lax.ppermute(right, "col", ring(col_count, 1))
    from_below = lax.ppermute(up, "row", ring(row_count, -1))
    from_above = lax.ppermute(down, "row", ring(row_count, 1))
    corner_shape = jax.ShapeDtypeStruct((6 * SUB, LANES), F32)
    corner_up, corner_down = pl.pallas_call(
        corner_kernel,
        in_specs=[vmem] * 2,
        out_specs=[vmem] * 2,
        out_shape=[corner_shape, corner_shape],
        compiler_params=params,
        name="corners",
    )(from_right, from_left)
    corner_below = lax.ppermute(corner_up, "row", ring(row_count, -1))
    corner_above = lax.ppermute(corner_down, "row", ring(row_count, 1))
    planes = CELL * CELL

    def stack(count):
        return (count, 2, er + 2 * BASE, LANES)

    plane_shape = jax.ShapeDtypeStruct(stack(planes), F32)
    noise_shape = jax.ShapeDtypeStruct(stack(PHASES * 4), F32)
    natural_shape = jax.ShapeDtypeStruct((4 * tiles, tile_rows + 2 * HALO, LANES), F32)
    order_scratch = pltpu.SMEM(colour_order.shape, I32)
    noise, natural = pl.pallas_call(
        functools.partial(noise_kernel, tile_rows, tile_cols),
        in_specs=[hbm] * 6,
        out_specs=[vmem] * 2,
        out_shape=[noise_shape, natural_shape],
        scratch_shapes=[
            order_scratch,
            pltpu.SMEM(seeds.shape, I32),
            pltpu.SemaphoreType.DMA((4 * tiles + 2,)),
        ],
        compiler_params=params,
        cost_estimate=estimate(4_000_000),
        name="noise",
    )(order, seeds, *sources)
    *state, _ = pl.pallas_call(
        functools.partial(planes_kernel, tile_rows, tile_cols),
        in_specs=[vmem] * 5,
        out_specs=[vmem] * 5,
        out_shape=[plane_shape] * 4 + [natural_shape],
        input_output_aliases={0: 4},
        compiler_params=params,
        cost_estimate=estimate(4_000_000),
        name="planes",
    )(natural, from_below, from_above, from_right, from_left)
    result, energy, *_ = pl.pallas_call(
        functools.partial(sweep_kernel, tile_rows, tile_cols, nodes),
        in_specs=[hbm] + [vmem] * 11,
        out_specs=[vmem] * 7,
        out_shape=[
            jax.ShapeDtypeStruct((tile_rows, tile_cols), F32),
            jax.ShapeDtypeStruct((devices, LANES), F32),
        ]
        + [plane_shape] * 4
        + [noise_shape],
        input_output_aliases={1 + i: 2 + i for i in range(5)},
        scratch_shapes=[
            pltpu.VMEM(stack(planes), F32),
            pltpu.VMEM(stack(planes), F32),
            pltpu.VMEM((PHASES + 1, SUB, LANES), F32),
            pltpu.VMEM((tiles, tile_rows, LANES), F32),
            order_scratch,
            pltpu.SMEM((8, SUB, LANES), F32),
            pltpu.SemaphoreType.DMA((9,)),
        ],
        compiler_params=params,
        cost_estimate=estimate(8_000_000),
        name="sweeps",
    )(
        order, *state, noise,
        from_below, from_above, from_right, from_left, corner_below, corner_above,
    )
    shared = lax.all_to_all(energy, AXES, 0, 0, tiled=True)
    energies = jnp.sum(shared, axis=0)[:PHASES].reshape(SWEEPS, COLOURS, chains)
    return (result[None], energies)


def solution(mesh):
    placed = (
        P(None, "row", "col"),
        P("row", "col"),
        P("row", "col"),
        P("row", "col"),
        P("row", "col", None, None, None),
        P(),
    )
    return jax.shard_map(
        local, mesh=mesh, in_specs=placed, out_specs=(P(None, "row", "col"), P()), check_vma=False
    )
```

```python
import functools

import jax
import jax.numpy as jnp
from jax import lax
from jax.experimental import pallas as pl
from jax.experimental.pallas import tpu as pltpu
from jax.sharding import PartitionSpec as P


SWEEPS = 2
COLOURS = 4
PHASES = SWEEPS * COLOURS
HALO = 2 * PHASES
CELL = 4
HC = HALO // CELL
LANES = 128
SUB = 8
GROUP = LANES // CELL
AXES = ("row", "col")
F32 = jnp.float32
I32 = jnp.int32

unit_step = 1.0 / 8388608.0
mix_factor = 73244475
SEED_BASE = 32768

SIN_COEFFS = (
    6.283185306485777,
    -41.34170192921984,
    81.60520938153618,
    -76.70366601553475,
    41.99996083008805,
    -14.336855962945094,
)


def lane_iota(shape):
    return lax.broadcasted_iota(I32, shape, len(shape) - 1)


def sub_iota(shape):
    return lax.broadcasted_iota(I32, shape, len(shape) - 2)


def lane_gather(value, index):
    return jnp.take_along_axis(value, index, axis=1, mode="promise_in_bounds")


def lroll(value, amount):
    amount = amount % value.shape[1]
    return pltpu.roll(value, amount, 1) if amount else value


SLOT = 8


def slot_gather(value, left):
    wide = lane_iota(value.shape)
    at = (wide + SLOT // 2) % LANES if left else wide
    index = CELL * (at % CELL) + (at % GROUP) // SLOT
    return lane_gather(value, index + (LANES - HALO if left else 0))


def lane_group(left):
    lane = lane_iota((SUB, LANES))
    return ((lane + SLOT // 2) % LANES if left else lane) // GROUP


def pick_group(group, values):
    result = values[0]
    for g in range(1, CELL):
        result = jnp.where(group == g, values[g], result)
    return result


def join_sides(right, left):
    return jnp.where(lane_iota(right.shape) % SLOT < SLOT // 2, right, left)


def pack_kernel(seeds_ref, *refs):
    sources, (up_ref, down_ref, left_ref, right_ref) = refs[:4], refs[4:8]
    edges, seeds_buf, sems = refs[8:]
    rows, cols = sources[0].shape
    mr = rows // CELL
    copies = []

    def copy(source, target):
        made = pltpu.make_async_copy(source, target, sems.at[len(copies)])
        made.start()
        copies.append(made)

    copy(seeds_ref, seeds_buf)
    for a, source in enumerate(sources):
        copy(source.at[:, pl.ds(0, LANES)], edges.at[2 * a])
        copy(source.at[:, pl.ds(cols - LANES, LANES)], edges.at[2 * a + 1])
    for a, source in enumerate(sources):
        copy(source.at[pl.ds(0, HALO)], up_ref.at[pl.ds(a * HALO, HALO)])
        copy(source.at[pl.ds(rows - HALO, HALO)], down_ref.at[pl.ds(a * HALO, HALO)])
    for made in copies:
        made.wait()
    for sweep in range(SWEEPS):
        seeds = seeds_buf[0, 0, sweep]
        high = (seeds // SEED_BASE).astype(F32)
        low = (seeds % SEED_BASE).astype(F32)
        for out in (left_ref, right_ref):
            base = out.shape[0] - SUB
            out[base + sweep : base + sweep + 1, 0:COLOURS] = high
            out[base + SWEEPS + sweep : base + SWEEPS + sweep + 1, 0:COLOURS] = low

    def pack(a, carry):
        for edge, out in ((0, left_ref), (1, right_ref)):
            group = lane_group(edge == 1)
            for r in range(CELL):
                value = slot_gather(edges[2 * a + edge, pl.ds(r, mr, stride=CELL), :], edge == 1)
                parts = [value[SUB * g : SUB * (g + 1)] for g in range(CELL)]
                at = pl.multiple_of((a * CELL + r) * SUB, SUB)
                out[pl.ds(at, SUB), :] = pick_group(group, parts)
        return carry

    lax.fori_loop(0, 4, pack, 0)


def corner_kernel(right_ref, left_ref, own_ref, after_ref, up_ref, down_ref):
    del after_ref
    group = lane_group(True)
    for a in range(4):
        sides = []
        for r in range(CELL):
            rows = slice((a * CELL + r) * SUB, (a * CELL + r + 1) * SUB)
            sides.append(join_sides(right_ref[rows, :], left_ref[rows, :]))
        rows = slice(a * SUB, (a + 1) * SUB)
        up_ref[rows, :] = pick_group(group, [lroll(v, GROUP * r) for r, v in enumerate(sides)])
        down_ref[rows, :] = pick_group(
            group, [lroll(v, GROUP * (r + 1)) for r, v in enumerate(sides)]
        )
    base = right_ref.shape[0] - SUB
    for out in (up_ref, down_ref):
        for i, source in enumerate((right_ref, left_ref, own_ref)):
            out[(4 + i) * SUB : (5 + i) * SUB, :] = source[base : base + SUB, :]


def scramble(hashed):
    sixteen = jnp.full_like(hashed, 16)
    hashed = hashed ^ lax.shift_right_logical(hashed, sixteen)
    hashed = hashed * mix_factor
    hashed = hashed ^ lax.shift_right_logical(hashed, sixteen)
    hashed = hashed * mix_factor
    return hashed ^ lax.shift_right_logical(hashed, sixteen)


def gaussian(first):
    nine = jnp.full_like(first, 9)
    one = lax.shift_right_logical(scramble(first), nine).astype(F32)
    two = lax.shift_right_logical(scramble(first + 1), nine).astype(F32)
    u1 = (one + 1.0) * unit_step
    v = 0.25 - jnp.abs(two * unit_step - 0.5)
    square = v * v
    poly = jnp.full_like(v, SIN_COEFFS[-1])
    for coeff in SIN_COEFFS[-2::-1]:
        poly = poly * square + coeff
    square = -2.0 * jnp.log(u1)
    return square * lax.rsqrt(jnp.maximum(square, 1e-30)) * (-(v * poly))


BASE = SUB


def rows_at(first, count):
    return pl.ds(BASE + first, count)


def lane_shift(value, amount, edge):
    moved = pltpu.roll(value, amount, 2)
    other = jnp.concatenate([moved[1:2], moved[0:1]], axis=0)
    return jnp.where(lane_iota(value.shape) == edge, other, moved)


def fold(value):
    count = value.shape[0]
    sub = sub_iota((SUB, LANES))
    total = jnp.where(sub >= HC, value[0:SUB], value[count - SUB : count])
    for top in range(SUB, count - SUB, SUB):
        total = total + value[top : top + SUB]
    return total


def gather_cells(value):
    wide = lane_iota(value.shape)
    return lane_gather(value, CELL * (wide % GROUP) + wide // GROUP)


def scatter_cells(value):
    wide = lane_iota(value.shape)
    return lane_gather(value, GROUP * (wide % CELL) + wide // CELL)


def column_planes(pieces):
    group = lane_iota(pieces[0].shape) // GROUP
    turned = [lroll(gather_cells(piece), GROUP * t) for t, piece in enumerate(pieces)]
    return [
        lroll(pick_group(group, [turned[(g - c) % CELL] for g in range(CELL)]), -GROUP * c)
        for c in range(CELL)
    ]


def natural_columns(planes):
    group = lane_iota(planes[0].shape) // GROUP
    turned = [lroll(plane, GROUP * c) for c, plane in enumerate(planes)]
    return [
        scatter_cells(
            lroll(pick_group(group, [turned[(g - t) % CELL] for g in range(CELL)]), -GROUP * t)
        )
        for t in range(CELL)
    ]


def put_ends(ref, plane, half, value):
    count = ref.shape[2] - 2 * BASE
    ref[plane, half, pl.ds(BASE + count - HC, HC), :] = value[0:HC]
    ref[plane, half, pl.ds(BASE, HC), :] = value[HC:SUB]


def node_offsets(tile_cols, row_cell, col_cell):
    return 2 * CELL * tile_cols * row_cell + 2 * CELL * col_cell


def phase_extra(colour, n, tile_cols):
    row, col = 2 * (colour // 2) + n // 2, 2 * (colour % 2) + n % 2
    return 2 * (row * tile_cols + col)


def noise_kernel(
    tile_rows, tile_cols,
    order_ref, seeds_ref, x_ref, b_ref, kappa_ref, mass_ref,
    Z, nat,
    order, seeds, sems,
):
    mr = tile_rows // CELL
    tiles = tile_cols // LANES
    copies = []

    def copy(source, target):
        made = pltpu.make_async_copy(source, target, sems.at[len(copies)])
        made.start()
        copies.append(made)

    copy(order_ref, order)
    copy(seeds_ref, seeds)
    for a, source in enumerate((x_ref, b_ref, kappa_ref, mass_ref)):
        for t in range(tiles):
            copy(source.at[:, pl.ds(t * LANES, LANES)], nat.at[a * tiles + t])
    copies[0].wait()
    copies[1].wait()
    offset_main = node_offsets(tile_cols, sub_iota((mr, LANES)), lane_iota((mr, LANES)))

    def noise_phase(phase, carry):
        own = seeds[0, 0, phase // COLOURS, 0, phase % COLOURS]
        colour = order[phase % COLOURS]
        for n in range(4):
            start = own + phase_extra(colour, n, tile_cols)
            Z[phase * 4 + n, 0, rows_at(HC, mr), :] = gaussian(offset_main + start)
        return carry

    lax.fori_loop(0, PHASES, noise_phase, 0)
    for made in copies[2:]:
        made.wait()


def planes_kernel(tile_rows, tile_cols, nat, right_ref, left_ref, X, B, S, I):
    mr = tile_rows // CELL
    tiles = tile_cols // LANES

    def row(r, carry):
        inner, outer = [], []
        for a in range(4):
            inner.append(
                column_planes(
                    [nat[a * tiles + t, pl.ds(r, mr, stride=CELL), :] for t in range(tiles)]
                )
            )
            rows = pl.ds(pl.multiple_of((a * CELL + r) * SUB, SUB), SUB)
            side = join_sides(right_ref[rows, :], left_ref[rows, :])
            outer.append([lroll(side, -SLOT * slot) for slot in range(LANES // SLOT)])
        for c in range(CELL):
            plane = r * CELL + c
            X[plane, 0, rows_at(HC, mr), :] = inner[0][c]
            B[plane, 0, rows_at(HC, mr), :] = inner[1][c]
            S[plane, 0, rows_at(HC, mr), :] = inner[2][c] * inner[3][c] + 4.0
            I[plane, 0, rows_at(HC, mr), :] = 1.0 / inner[3][c]
            for g in range(CELL):
                slot = CELL * g + c
                at = rows_at(HC + SUB * g, SUB)
                X[plane, 1, at, :] = outer[0][slot]
                B[plane, 1, at, :] = outer[1][slot]
                S[plane, 1, at, :] = outer[2][slot] * outer[3][slot] + 4.0
                I[plane, 1, at, :] = 1.0 / outer[3][slot]
        return carry

    lax.fori_loop(0, CELL, row, 0)


def sweep_kernel(
    tile_rows, tile_cols, nodes,
    order_ref, x_in, b_in, s_in, i_in, z_in,
    below_ref, above_ref, right_ref, left_ref, cbelow_ref, cabove_ref,
    out_ref, energy_ref, X, B, S, I, Z,
    strip, W, D, EN, nat, order, around, sems,
):
    del x_in, b_in, s_in, i_in, z_in
    copies = []

    def copy(source, target):
        made = pltpu.make_async_copy(source, target, sems.at[len(copies)])
        made.start()
        copies.append(made)

    copy(order_ref, order)
    for at, (ref, back) in enumerate((
        (right_ref, 1), (left_ref, 1), (cabove_ref, 1), (cbelow_ref, 1),
        (cabove_ref, 3), (cabove_ref, 2), (cbelow_ref, 3), (cbelow_ref, 2),
    )):
        top = ref.shape[0] - back * SUB
        copy(ref.at[pl.ds(top, SUB), pl.ds(0, LANES)], around.at[at])
    mr = tile_rows // CELL
    er = mr + 2 * HC
    tiles = tile_cols // LANES
    lane = lane_iota((SUB, LANES))
    sub = sub_iota((SUB, LANES))
    low = sub < HC

    corner = []
    for a in range(4):
        at = slice(a * SUB, (a + 1) * SUB)
        corner.append(jnp.where(low, cbelow_ref[at, :], cabove_ref[at, :]))

    def strips(a, carry):
        for t in range(tiles):
            lanes = slice(t * LANES, (t + 1) * LANES)
            at = pl.ds(pl.multiple_of(a * HALO, HALO), HALO)
            for start, source in ((0, below_ref), (HALO, above_ref)):
                strip[a * tiles + t, start : start + HALO, :] = source[at, lanes]
        return carry

    lax.fori_loop(0, 4, strips, 0)

    def ends(r, carry):
        inner = [
            column_planes(
                [strip[a * tiles + t, pl.ds(r, SUB, stride=CELL), :] for t in range(tiles)]
            )
            for a in range(4)
        ]
        for c in range(CELL):
            plane = r * CELL + c
            amount = (2 * LANES - GROUP * r - SLOT * c) % LANES
            outer = [pltpu.roll(value, amount, 1) for value in carry]
            for half, value in enumerate(([v[c] for v in inner], outer)):
                put_ends(X, plane, half, value[0])
                put_ends(B, plane, half, value[1])
                put_ends(S, plane, half, value[2] * value[3] + 4.0)
                put_ends(I, plane, half, 1.0 / value[3])
        return carry

    lax.fori_loop(0, CELL // 2, lambda i, carry: ends(2 * i + 1, ends(2 * i, carry)), tuple(corner))

    every = rows_at(0, er)

    def start(r, energy):
        above, up = (r + CELL - 1) % CELL, jnp.where(r == 0, -1, 0)
        below, down = (r + 1) % CELL, jnp.where(r == CELL - 1, 1, 0)
        field = [X[r * CELL + c, :, every, :] for c in range(CELL)]
        inv = [I[r * CELL + c, :, every, :] for c in range(CELL)]

        def around_sum(ref, value, c):
            left = value[c - 1] if c else lane_shift(value[CELL - 1], 1, 0)
            right = value[c + 1] if c < CELL - 1 else lane_shift(value[0], LANES - 1, LANES - 1)
            return (
                ref[above * CELL + c, :, rows_at(up, er), :]
                + ref[below * CELL + c, :, rows_at(down, er), :]
                + left
                + right
            )

        for c in range(CELL):
            plane = r * CELL + c
            stiff = S[plane, :, every, :]
            first = stiff * field[c] - around_sum(X, field, c)
            scaled = inv[c] * first
            W[plane, :, every, :] = scaled
            D[plane, :, every, :] = stiff * stiff * inv[c] + around_sum(I, inv, c)
            part = 0.5 * scaled[0] * first[0] - B[plane, 0, every, :] * field[c][0]
            energy = energy + fold(part)
        return energy

    EN[0] = lax.fori_loop(0, CELL, start, jnp.zeros((SUB, LANES), F32))

    for made in copies:
        made.wait()
    spot = lane % GROUP
    is_right = spot < GROUP // 2
    in_right_corner = (lane >= 2 * HC) & (lane < 3 * HC)
    in_left_corner = (lane >= HC) & (lane < 2 * HC)
    end_cell = jnp.where(low, sub, sub + mr - 2 * HC)
    side_row = SUB * jnp.where(is_right, lane // GROUP, (lane // GROUP + 1) % CELL) + sub
    side_row = jnp.where(in_right_corner | in_left_corner, end_cell, side_row)
    side_col = jnp.where(is_right, spot, spot + LANES - GROUP)
    side_col = jnp.where(in_right_corner, lane - 2 * HC, side_col)
    side_col = jnp.where(in_left_corner, lane + LANES - 2 * HC, side_col)
    offset_side = node_offsets(tile_cols, side_row, side_col)
    offset_ends = node_offsets(tile_cols, end_cell, lane)

    def run_phase(phase, carry):
        sweep, k = phase // COLOURS, phase % COLOURS
        colour = order[k]
        ci, cj = colour // 2, colour % 2
        r0, c0 = 2 * ci, 2 * cj

        def seed(at):
            return around[at, sweep, k].astype(I32) * SEED_BASE + around[
                at, SWEEPS + sweep, k
            ].astype(I32)

        ends_seed = offset_ends + jnp.where(low, seed(3), seed(2))
        side_seed = jnp.where(is_right, seed(0), seed(1))
        side_seed = jnp.where(in_right_corner, jnp.where(low, seed(6), seed(4)), side_seed)
        side_seed = jnp.where(in_left_corner, jnp.where(low, seed(7), seed(5)), side_seed)
        side_seed = offset_side + side_seed
        for n in range(4):
            at = phase * 4 + n
            extra = phase_extra(colour, n, tile_cols)
            put_ends(Z, at, 0, gaussian(ends_seed + extra))
            value = gaussian(side_seed + extra)
            for g in range(mr // SUB):
                Z[at, 1, rows_at(HC + SUB * g, SUB), :] = lroll(value, -GROUP * g)
            put_ends(Z, at, 1, lroll(value, -2 * HC))
        z = [Z[phase * 4 + n, :, every, :] for n in range(4)]

        own = [(r0 + n // 2) * CELL + c0 + n % 2 for n in range(4)]
        above, up = (r0 + CELL - 1) % CELL, ci - 1
        below, down = (r0 + 2) % CELL, ci
        left, right = (c0 + CELL - 1) % CELL, (c0 + 2) % CELL
        above_rows, below_rows = rows_at(up, er), rows_at(down, er)
        w_own = [W[plane, :, every, :] for plane in own]
        w_above = [W[above * CELL + c0 + i, :, above_rows, :] for i in range(2)]
        w_below = [W[below * CELL + c0 + i, :, below_rows, :] for i in range(2)]
        w_left = [
            lane_shift(W[(r0 + i) * CELL + left, :, every, :], 1 - cj, -cj) for i in range(2)
        ]
        w_right = [
            lane_shift(
                W[(r0 + i) * CELL + right, :, every, :], (LANES - 1) * cj, LANES * cj - 1
            )
            for i in range(2)
        ]
        inv = [I[plane, :, every, :] for plane in own]
        stiff = [S[plane, :, every, :] for plane in own]
        sums = [
            w_above[0] + w_own[2] + w_left[0] + w_own[1],
            w_above[1] + w_own[3] + w_own[0] + w_right[0],
            w_own[0] + w_below[0] + w_left[1] + w_own[3],
            w_own[1] + w_below[1] + w_own[2] + w_right[1],
        ]
        residual = [
            B[own[n], :, every, :] - (stiff[n] * w_own[n] - sums[n]) for n in range(4)
        ]
        scaled = [stiff[n] * inv[n] for n in range(4)]
        diag = [D[plane, :, every, :] for plane in own]
        m01, m02 = -(scaled[0] + scaled[1]), -(scaled[0] + scaled[2])
        m13, m23 = -(scaled[1] + scaled[3]), -(scaled[2] + scaled[3])
        m03, m12 = inv[1] + inv[2], inv[0] + inv[3]
        q0 = lax.rsqrt(diag[0])
        l10, l20, l30 = m01 * q0, m02 * q0, m03 * q0
        q1 = lax.rsqrt(diag[1] - l10 * l10)
        l21, l31 = (m12 - l20 * l10) * q1, (m13 - l30 * l10) * q1
        q2 = lax.rsqrt(diag[2] - l20 * l20 - l21 * l21)
        l32 = (m23 - l30 * l20 - l31 * l21) * q2
        q3 = lax.rsqrt(diag[3] - l30 * l30 - l31 * l31 - l32 * l32)
        f0 = residual[0] * q0
        f1 = (residual[1] - l10 * f0) * q1
        f2 = (residual[2] - l20 * f0 - l21 * f1) * q2
        f3 = (residual[3] - l30 * f0 - l31 * f1 - l32 * f2) * q3
        y0, y1, y2, y3 = f0 + z[0], f1 + z[1], f2 + z[2], f3 + z[3]
        d3 = y3 * q3
        d2 = (y2 - l32 * d3) * q2
        d1 = (y1 - l21 * d2 - l31 * d3) * q1
        d0 = (y0 - l10 * d1 - l20 * d2 - l30 * d3) * q0
        delta = [d0, d1, d2, d3]
        for n in range(4):
            X[own[n], 0, every, :] = X[own[n], 0, every, :] + delta[n][0]
        change = 0.0
        for n, f in enumerate((f0, f1, f2, f3)):
            change = change + (z[n][0] * z[n][0] - f[0] * f[0])
        EN[phase + 1] = 0.5 * fold(change)
        for n, (across, beside) in enumerate(((1, 2), (0, 3), (3, 0), (2, 1))):
            step = stiff[n] * delta[n] - (delta[across] + delta[beside])
            W[own[n], :, every, :] = w_own[n] + inv[n] * step

        def spread(plane, rows, value):
            W[plane, :, rows, :] = W[plane, :, rows, :] - I[plane, :, rows, :] * value

        for i in range(2):
            spread(above * CELL + c0 + i, above_rows, delta[i])
            spread(below * CELL + c0 + i, below_rows, delta[2 + i])
            spread(
                (r0 + i) * CELL + left, every,
                lane_shift(delta[2 * i], (LANES - 1) * (1 - cj), LANES * (1 - cj) - 1),
            )
            spread(
                (r0 + i) * CELL + right, every, lane_shift(delta[2 * i + 1], cj, cj - 1)
            )
        return carry

    lax.fori_loop(0, PHASES, run_phase, 0)

    running = EN[0]
    result = jnp.zeros((1, LANES), F32)
    first_row = lane_iota((1, LANES))
    for phase in range(PHASES):
        if phase:
            running = running + EN[phase]
        total = jnp.sum(jnp.sum(running, axis=0, keepdims=True), axis=1, keepdims=True)
        result = jnp.where(first_row == phase, total, result)
    energy_ref[...] = jnp.broadcast_to(result / nodes, energy_ref.shape)

    def restore(i, carry):
        for r in (2 * i, 2 * i + 1):
            columns = natural_columns(
                [X[r * CELL + c, 0, rows_at(HC, mr), :] for c in range(CELL)]
            )
            for t, value in enumerate(columns):
                nat[t, pl.ds(r, mr, stride=CELL), :] = value
        return carry

    lax.fori_loop(0, CELL // 2, restore, 0)
    for t in range(tiles):
        out_ref[:, t * LANES : (t + 1) * LANES] = nat[t]


def ring(count, step):
    return [(i, (i + step) % count) for i in range(count)]


def estimate(flops):
    return pl.CostEstimate(flops=flops, bytes_accessed=1_000_000, transcendentals=0)


def local(initial_field, information, kappa_squared, lumped_mass, noise_seeds, colour_order):
    chains, tile_rows, tile_cols = initial_field.shape
    row_count, col_count = lax.axis_size("row"), lax.axis_size("col")
    devices = row_count * col_count
    nodes = tile_rows * row_count * tile_cols * col_count
    mr = tile_rows // CELL
    er = mr + 2 * HC
    tiles = tile_cols // LANES
    vmem = pl.BlockSpec(memory_space=pltpu.VMEM)
    hbm = pl.BlockSpec(memory_space=pltpu.HBM)
    params = pltpu.CompilerParams(vmem_limit_bytes=16 * 1024 * 1024)

    def in_hbm(value):
        return pltpu.with_memory_space_constraint(value, pltpu.HBM)

    seeds = in_hbm(jnp.swapaxes(noise_seeds, 3, 4))
    order = in_hbm(colour_order)
    sources = [
        in_hbm(value) for value in (initial_field[0], information, kappa_squared, lumped_mass)
    ]
    rows_shape = jax.ShapeDtypeStruct((4 * HALO, tile_cols), F32)
    cols_shape = jax.ShapeDtypeStruct((4 * CELL * SUB + SUB, LANES), F32)
    up, down, left, right = pl.pallas_call(
        pack_kernel,
        in_specs=[hbm] * 5,
        out_specs=[vmem] * 4,
        out_shape=[rows_shape, rows_shape, cols_shape, cols_shape],
        scratch_shapes=[
            pltpu.VMEM((8, tile_rows, LANES), F32),
            pltpu.VMEM(seeds.shape, I32),
            pltpu.SemaphoreType.DMA((17,)),
        ],
        compiler_params=params,
        name="pack",
    )(seeds, *sources)
    from_right = lax.ppermute(left, "col", ring(col_count, -1))
    from_left = lax.ppermute(right, "col", ring(col_count, 1))
    from_below = lax.ppermute(up, "row", ring(row_count, -1))
    from_above = lax.ppermute(down, "row", ring(row_count, 1))
    planes = CELL * CELL

    def stack(count):
        return (count, 2, er + 2 * BASE, LANES)

    plane_shape = jax.ShapeDtypeStruct(stack(planes), F32)
    noise_shape = jax.ShapeDtypeStruct(stack(PHASES * 4), F32)
    natural_shape = jax.ShapeDtypeStruct((4 * tiles, tile_rows, LANES), F32)
    order_scratch = pltpu.SMEM(colour_order.shape, I32)
    noise, natural = pl.pallas_call(
        functools.partial(noise_kernel, tile_rows, tile_cols),
        in_specs=[hbm] * 6,
        out_specs=[vmem] * 2,
        out_shape=[noise_shape, natural_shape],
        scratch_shapes=[
            order_scratch,
            pltpu.SMEM(seeds.shape, I32),
            pltpu.SemaphoreType.DMA((4 * tiles + 2,)),
        ],
        compiler_params=params,
        cost_estimate=estimate(4_000_000),
        name="noise",
    )(order, seeds, *sources)
    corner_shape = jax.ShapeDtypeStruct((7 * SUB, LANES), F32)
    corner_up, corner_down = pl.pallas_call(
        corner_kernel,
        in_specs=[vmem] * 3 + [pl.BlockSpec(memory_space=pl.ANY)],
        out_specs=[vmem] * 2,
        out_shape=[corner_shape, corner_shape],
        compiler_params=params,
        name="corners",
    )(from_right, from_left, left, noise)
    corner_below = lax.ppermute(corner_up, "row", ring(row_count, -1))
    corner_above = lax.ppermute(corner_down, "row", ring(row_count, 1))
    state = pl.pallas_call(
        functools.partial(planes_kernel, tile_rows, tile_cols),
        in_specs=[vmem] * 3,
        out_specs=[vmem] * 4,
        out_shape=[plane_shape] * 4,
        compiler_params=params,
        cost_estimate=estimate(4_000_000),
        name="planes",
    )(natural, from_right, from_left)
    result, energy, *_ = pl.pallas_call(
        functools.partial(sweep_kernel, tile_rows, tile_cols, nodes),
        in_specs=[hbm] + [vmem] * 11,
        out_specs=[vmem] * 7,
        out_shape=[
            jax.ShapeDtypeStruct((tile_rows, tile_cols), F32),
            jax.ShapeDtypeStruct((devices, LANES), F32),
        ]
        + [plane_shape] * 4
        + [noise_shape],
        input_output_aliases={1 + i: 2 + i for i in range(5)},
        scratch_shapes=[
            pltpu.VMEM((4 * tiles, 2 * HALO, LANES), F32),
            pltpu.VMEM(stack(planes), F32),
            pltpu.VMEM(stack(planes), F32),
            pltpu.VMEM((PHASES + 1, SUB, LANES), F32),
            pltpu.VMEM((tiles, tile_rows, LANES), F32),
            order_scratch,
            pltpu.SMEM((8, SUB, LANES), F32),
            pltpu.SemaphoreType.DMA((9,)),
        ],
        compiler_params=params,
        cost_estimate=estimate(8_000_000),
        name="sweeps",
    )(
        order, *state, noise,
        from_below, from_above, from_right, from_left, corner_below, corner_above,
    )
    shared = lax.all_to_all(energy, AXES, 0, 0, tiled=True)
    energies = jnp.sum(shared, axis=0)[:PHASES].reshape(SWEEPS, COLOURS, chains)
    return (result[None], energies)


def solution(mesh):
    placed = (
        P(None, "row", "col"),
        P("row", "col"),
        P("row", "col"),
        P("row", "col"),
        P("row", "col", None, None, None),
        P(),
    )
    return jax.shard_map(
        local, mesh=mesh, in_specs=placed, out_specs=(P(None, "row", "col"), P()), check_vma=False
    )
```

```python
import functools

import jax
import jax.numpy as jnp
from jax import lax
from jax.experimental import pallas as pl
from jax.experimental.pallas import tpu as pltpu
from jax.sharding import PartitionSpec as P


SWEEPS = 2
COLOURS = 4
PHASES = SWEEPS * COLOURS
HALO = 2 * PHASES
CELL = 4
HC = HALO // CELL
LANES = 128
SUB = 8
GROUP = LANES // CELL
AXES = ("row", "col")
F32 = jnp.float32
I32 = jnp.int32

unit_step = 1.0 / 8388608.0
mix_factor = 73244475
SEED_BASE = 32768

SIN_COEFFS = (
    -6.283185159611163,
    41.3416549293435,
    -81.60099819261265,
    76.54965682062002,
    -39.535813711455276,
)


def lane_iota(shape):
    return lax.broadcasted_iota(I32, shape, len(shape) - 1)


def sub_iota(shape):
    return lax.broadcasted_iota(I32, shape, len(shape) - 2)


def lane_gather(value, index):
    return jnp.take_along_axis(value, index, axis=1, mode="promise_in_bounds")


def lroll(value, amount):
    amount = amount % value.shape[1]
    return pltpu.roll(value, amount, 1) if amount else value


SLOT = 8


def slot_gather(value, left):
    wide = lane_iota(value.shape)
    at = (wide + SLOT // 2) % LANES if left else wide
    index = CELL * (at % CELL) + (at % GROUP) // SLOT
    return lane_gather(value, index + (LANES - HALO if left else 0))


def lane_group(left):
    lane = lane_iota((SUB, LANES))
    return ((lane + SLOT // 2) % LANES if left else lane) // GROUP


def pick_group(group, values):
    result = values[0]
    for g in range(1, CELL):
        result = jnp.where(group == g, values[g], result)
    return result


def join_sides(right, left):
    return jnp.where(lane_iota(right.shape) % SLOT < SLOT // 2, right, left)


def pack_kernel(order_ref, seeds_ref, *refs):
    sources, (up_ref, down_ref, left_ref, right_ref, order_out, seeds_buf) = refs[:4], refs[4:10]
    edges, sems = refs[10:]
    rows, cols = sources[0].shape
    mr = rows // CELL
    copies = []

    def copy(source, target):
        made = pltpu.make_async_copy(source, target, sems.at[len(copies)])
        made.start()
        copies.append(made)

    copy(seeds_ref, seeds_buf)
    copy(order_ref, order_out)
    for a, source in enumerate(sources):
        copy(source.at[:, pl.ds(0, LANES)], edges.at[2 * a])
        copy(source.at[:, pl.ds(cols - LANES, LANES)], edges.at[2 * a + 1])
    for a, source in enumerate(sources):
        copy(source.at[pl.ds(0, HALO)], up_ref.at[pl.ds(a * HALO, HALO)])
        copy(source.at[pl.ds(rows - HALO, HALO)], down_ref.at[pl.ds(a * HALO, HALO)])
    for made in copies:
        made.wait()
    for sweep in range(SWEEPS):
        seeds = seeds_buf[0, 0, sweep]
        high = (seeds // SEED_BASE).astype(F32)
        low = (seeds % SEED_BASE).astype(F32)
        for out in (left_ref, right_ref):
            base = out.shape[0] - SUB
            out[base + sweep : base + sweep + 1, 0:COLOURS] = high
            out[base + SWEEPS + sweep : base + SWEEPS + sweep + 1, 0:COLOURS] = low

    def pack(a, carry):
        for edge, out in ((0, left_ref), (1, right_ref)):
            group = lane_group(edge == 1)
            for r in range(CELL):
                value = slot_gather(edges[2 * a + edge, pl.ds(r, mr, stride=CELL), :], edge == 1)
                parts = [value[SUB * g : SUB * (g + 1)] for g in range(CELL)]
                at = pl.multiple_of((a * CELL + r) * SUB, SUB)
                out[pl.ds(at, SUB), :] = pick_group(group, parts)
        return carry

    lax.fori_loop(0, 4, pack, 0)


def half_turn(value):
    return pltpu.roll(value, SUB // 2, 0)


def corner_kernel(right_ref, left_ref, own_ref, after_ref, up_ref, down_ref):
    del after_ref
    group = lane_group(True)
    low = sub_iota((SUB, LANES)) < HC
    ups, downs = [], []
    for a in range(4):
        sides = []
        for r in range(CELL):
            rows = slice((a * CELL + r) * SUB, (a * CELL + r + 1) * SUB)
            sides.append(join_sides(right_ref[rows, :], left_ref[rows, :]))
        ups.append(pick_group(group, [lroll(v, GROUP * r) for r, v in enumerate(sides)]))
        downs.append(pick_group(group, [lroll(v, GROUP * (r + 1)) for r, v in enumerate(sides)]))
    for pair in range(2):
        rows = slice(pair * SUB, (pair + 1) * SUB)
        up_ref[rows, :] = jnp.where(low, ups[2 * pair], half_turn(ups[2 * pair + 1]))
        down_ref[rows, :] = jnp.where(low, half_turn(downs[2 * pair + 1]), downs[2 * pair])
    base = right_ref.shape[0] - SUB
    for out in (up_ref, down_ref):
        for i, source in enumerate((right_ref, left_ref, own_ref)):
            out[2 * SUB : 2 * SUB + SUB // 2, i * SUB : i * SUB + COLOURS] = source[
                base : base + SUB // 2, 0:COLOURS
            ]


def scramble(hashed):
    sixteen = jnp.full_like(hashed, 16)
    hashed = hashed ^ lax.shift_right_logical(hashed, sixteen)
    hashed = hashed * mix_factor
    hashed = hashed ^ lax.shift_right_logical(hashed, sixteen)
    hashed = hashed * mix_factor
    return hashed ^ lax.shift_right_logical(hashed, sixteen)


def gaussian(first):
    nine = jnp.full_like(first, 9)
    one = lax.shift_right_logical(scramble(first), nine).astype(F32)
    two = lax.shift_right_logical(scramble(first + 1), nine).astype(F32)
    u1 = (one + 1.0) * unit_step
    v = 0.25 - jnp.abs(two * unit_step - 0.5)
    square = v * v
    poly = jnp.full_like(v, SIN_COEFFS[-1])
    for coeff in SIN_COEFFS[-2::-1]:
        poly = poly * square + coeff
    square = -2.0 * jnp.log(u1)
    return square * lax.rsqrt(jnp.maximum(square, 1e-30)) * (v * poly)


BASE = SUB


def rows_at(first, count):
    return pl.ds(BASE + first, count)


def lane_shift(value, amount, edge):
    moved = pltpu.roll(value, amount, 2)
    other = jnp.concatenate([moved[1:2], moved[0:1]], axis=0)
    return jnp.where(lane_iota(value.shape) == edge, other, moved)


def fold(value):
    count = value.shape[0]
    sub = sub_iota((SUB, LANES))
    total = jnp.where(sub >= HC, value[0:SUB], value[count - SUB : count])
    for top in range(SUB, count - SUB, SUB):
        total = total + value[top : top + SUB]
    return total


def gather_cells(value):
    wide = lane_iota(value.shape)
    return lane_gather(value, CELL * (wide % GROUP) + wide // GROUP)


def scatter_cells(value):
    wide = lane_iota(value.shape)
    return lane_gather(value, GROUP * (wide % CELL) + wide // CELL)


def column_planes(pieces):
    group = lane_iota(pieces[0].shape) // GROUP
    turned = [lroll(gather_cells(piece), GROUP * t) for t, piece in enumerate(pieces)]
    return [
        lroll(pick_group(group, [turned[(g - c) % CELL] for g in range(CELL)]), -GROUP * c)
        for c in range(CELL)
    ]


def natural_columns(planes):
    group = lane_iota(planes[0].shape) // GROUP
    turned = [lroll(plane, GROUP * c) for c, plane in enumerate(planes)]
    return [
        scatter_cells(
            lroll(pick_group(group, [turned[(g - t) % CELL] for g in range(CELL)]), -GROUP * t)
        )
        for t in range(CELL)
    ]


def put_ends(ref, plane, half, value):
    count = ref.shape[2] - 2 * BASE
    ref[plane, half, pl.ds(BASE + count - HC, HC), :] = value[0:HC]
    ref[plane, half, pl.ds(BASE, HC), :] = value[HC:SUB]


def node_offsets(tile_cols, row_cell, col_cell):
    return 2 * CELL * tile_cols * row_cell + 2 * CELL * col_cell


def phase_extra(colour, n, tile_cols):
    row, col = 2 * (colour // 2) + n // 2, 2 * (colour % 2) + n % 2
    return 2 * (row * tile_cols + col)


def noise_kernel(
    tile_rows, tile_cols,
    order_ref, seeds_ref, x_ref, b_ref, kappa_ref, mass_ref,
    Z, nat,
    order, seeds, sems,
):
    mr = tile_rows // CELL
    tiles = tile_cols // LANES
    copies = []

    def copy(source, target):
        made = pltpu.make_async_copy(source, target, sems.at[len(copies)])
        made.start()
        copies.append(made)

    copy(order_ref, order)
    copy(seeds_ref, seeds)
    for a, source in enumerate((x_ref, b_ref, kappa_ref, mass_ref)):
        for t in range(tiles):
            copy(source.at[:, pl.ds(t * LANES, LANES)], nat.at[a * tiles + t])
    copies[0].wait()
    copies[1].wait()
    offset_main = node_offsets(tile_cols, sub_iota((mr, LANES)), lane_iota((mr, LANES)))

    def noise_phase(phase, carry):
        own = seeds[0, 0, phase // COLOURS, 0, phase % COLOURS]
        colour = order[phase % COLOURS]
        for n in range(4):
            start = own + phase_extra(colour, n, tile_cols)
            Z[phase * 4 + n, 0, rows_at(HC, mr), :] = gaussian(offset_main + start)
        return carry

    lax.fori_loop(0, PHASES, noise_phase, 0)
    for made in copies[2:]:
        made.wait()


def planes_kernel(tile_rows, tile_cols, nat, right_ref, left_ref, X, B, S, I):
    mr = tile_rows // CELL
    tiles = tile_cols // LANES

    def row(r, carry):
        inner, outer = [], []
        for a in range(4):
            inner.append(
                column_planes(
                    [nat[a * tiles + t, pl.ds(r, mr, stride=CELL), :] for t in range(tiles)]
                )
            )
            rows = pl.ds(pl.multiple_of((a * CELL + r) * SUB, SUB), SUB)
            side = join_sides(right_ref[rows, :], left_ref[rows, :])
            outer.append([lroll(side, -SLOT * slot) for slot in range(LANES // SLOT)])
        for c in range(CELL):
            plane = r * CELL + c
            X[plane, 0, rows_at(HC, mr), :] = inner[0][c]
            B[plane, 0, rows_at(HC, mr), :] = inner[1][c]
            S[plane, 0, rows_at(HC, mr), :] = inner[2][c] * inner[3][c] + 4.0
            I[plane, 0, rows_at(HC, mr), :] = 1.0 / inner[3][c]
            for g in range(CELL):
                slot = CELL * g + c
                at = rows_at(HC + SUB * g, SUB)
                X[plane, 1, at, :] = outer[0][slot]
                B[plane, 1, at, :] = outer[1][slot]
                S[plane, 1, at, :] = outer[2][slot] * outer[3][slot] + 4.0
                I[plane, 1, at, :] = 1.0 / outer[3][slot]
        return carry

    lax.fori_loop(0, CELL, row, 0)


def sweep_kernel(
    tile_rows, tile_cols, nodes,
    order_ref, x_in, b_in, s_in, i_in, Z,
    below_ref, above_ref, right_ref, left_ref, cbelow_ref, cabove_ref,
    out_ref, energy_ref, X, B, S, I,
    strip, W, D, SH, DL, ZH, ZE, EN, nat, order, around, sems, out_sems,
):
    del x_in, b_in, s_in, i_in
    copies = []

    def copy(source, target):
        made = pltpu.make_async_copy(source, target, sems.at[len(copies)])
        made.start()
        copies.append(made)

    copy(order_ref, order)
    for at, ref in enumerate((right_ref, left_ref, cabove_ref, cbelow_ref)):
        copy(ref.at[pl.ds(ref.shape[0] - SUB, SUB)], around.at[at])
    mr = tile_rows // CELL
    er = mr + 2 * HC
    tiles = tile_cols // LANES
    lane = lane_iota((SUB, LANES))
    sub = sub_iota((SUB, LANES))
    low = sub < HC

    corner = []
    for pair in range(2):
        at = slice(pair * SUB, (pair + 1) * SUB)
        under, over = cbelow_ref[at, :], cabove_ref[at, :]
        corner.append(jnp.where(low, under, over))
        corner.append(half_turn(jnp.where(low, over, under)))

    def strips(a, carry):
        for t in range(tiles):
            lanes = slice(t * LANES, (t + 1) * LANES)
            at = pl.ds(pl.multiple_of(a * HALO, HALO), HALO)
            for start, source in ((0, below_ref), (HALO, above_ref)):
                strip[a * tiles + t, start : start + HALO, :] = source[at, lanes]
        return carry

    lax.fori_loop(0, 4, strips, 0)

    def ends(r, carry):
        inner = [
            column_planes(
                [strip[a * tiles + t, pl.ds(r, SUB, stride=CELL), :] for t in range(tiles)]
            )
            for a in range(4)
        ]
        for c in range(CELL):
            plane = r * CELL + c
            amount = (2 * LANES - GROUP * r - SLOT * c) % LANES
            outer = [pltpu.roll(value, amount, 1) for value in carry]
            for half, value in enumerate(([v[c] for v in inner], outer)):
                put_ends(X, plane, half, value[0])
                put_ends(B, plane, half, value[1])
                put_ends(S, plane, half, value[2] * value[3] + 4.0)
                put_ends(I, plane, half, 1.0 / value[3])
        return carry

    lax.fori_loop(0, CELL // 2, lambda i, carry: ends(2 * i + 1, ends(2 * i, carry)), tuple(corner))

    every = rows_at(0, er)

    def start(r, energy):
        above, up = (r + CELL - 1) % CELL, jnp.where(r == 0, -1, 0)
        below, down = (r + 1) % CELL, jnp.where(r == CELL - 1, 1, 0)
        field = [X[r * CELL + c, :, every, :] for c in range(CELL)]
        inv = [I[r * CELL + c, :, every, :] for c in range(CELL)]

        def around_sum(ref, value, c):
            left = value[c - 1] if c else lane_shift(value[CELL - 1], 1, 0)
            right = value[c + 1] if c < CELL - 1 else lane_shift(value[0], LANES - 1, LANES - 1)
            return (
                ref[above * CELL + c, :, rows_at(up, er), :]
                + ref[below * CELL + c, :, rows_at(down, er), :]
                + left
                + right
            )

        for c in range(CELL):
            plane = r * CELL + c
            stiff = S[plane, :, every, :]
            first = stiff * field[c] - around_sum(X, field, c)
            scaled = inv[c] * first
            W[plane, :, every, :] = scaled
            D[plane, :, every, :] = stiff * stiff * inv[c] + around_sum(I, inv, c)
            part = 0.5 * scaled[0] * first[0] - B[plane, 0, every, :] * field[c][0]
            energy = energy + fold(part)
        return energy

    EN[0] = lax.fori_loop(0, CELL, start, jnp.zeros((SUB, LANES), F32))

    for made in copies:
        made.wait()
    spot = lane % GROUP
    is_right = spot < GROUP // 2
    in_right_corner = (lane >= 2 * HC) & (lane < 3 * HC)
    in_left_corner = (lane >= HC) & (lane < 2 * HC)
    end_cell = jnp.where(low, sub, sub + mr - 2 * HC)
    side_row = SUB * jnp.where(is_right, lane // GROUP, (lane // GROUP + 1) % CELL) + sub
    side_row = jnp.where(in_right_corner | in_left_corner, end_cell, side_row)
    side_col = jnp.where(is_right, spot, spot + LANES - GROUP)
    side_col = jnp.where(in_right_corner, lane - 2 * HC, side_col)
    side_col = jnp.where(in_left_corner, lane + LANES - 2 * HC, side_col)
    offset_side = node_offsets(tile_cols, side_row, side_col)
    offset_ends = node_offsets(tile_cols, end_cell, lane)

    def halo_noise(phase):
        sweep, k = phase // COLOURS, phase % COLOURS
        colour = order[k]

        def seed(at, block):
            high = around[at, sweep, block * SUB + k].astype(I32)
            return high * SEED_BASE + around[at, SWEEPS + sweep, block * SUB + k].astype(I32)

        ends_seed = offset_ends + jnp.where(low, seed(3, 2), seed(2, 2))
        side_seed = jnp.where(is_right, seed(0, 0), seed(1, 0))
        ends = jnp.where(low, seed(3, 0), seed(2, 0))
        side_seed = jnp.where(in_right_corner, ends, side_seed)
        ends = jnp.where(low, seed(3, 1), seed(2, 1))
        side_seed = offset_side + jnp.where(in_left_corner, ends, side_seed)
        for n in range(4):
            extra = phase_extra(colour, n, tile_cols)
            at = (phase % 2) * 4 + n
            ZE[at] = half_turn(gaussian(ends_seed + extra))
            value = gaussian(side_seed + extra)
            for g in range(mr // SUB):
                ZH[at, HC + SUB * g : HC + SUB * (g + 1), :] = lroll(value, -GROUP * g)
            value = lroll(value, -2 * HC)
            ZH[at, er - HC : er, :] = value[0:HC]
            ZH[at, 0:HC, :] = value[HC:SUB]

    halo_noise(jnp.int32(0))

    def run_phase(phase, carry):
        colour = order[phase % COLOURS]
        ci, cj = colour // 2, colour % 2
        r0, c0 = 2 * ci, 2 * cj
        slot = (phase % 2) * 4
        z_ends = [ZE[slot + n] for n in range(4)]
        own = [(r0 + n // 2) * CELL + c0 + n % 2 for n in range(4)]
        above, up = (r0 + CELL - 1) % CELL, ci - 1
        below, down = (r0 + 2) % CELL, ci
        left, right = (c0 + CELL - 1) % CELL, (c0 + 2) % CELL
        above = [above * CELL + c0 + i for i in range(2)]
        below = [below * CELL + c0 + i for i in range(2)]
        left = [(r0 + i) * CELL + left for i in range(2)]
        right = [(r0 + i) * CELL + right for i in range(2)]
        for i in range(2):
            SH[i] = lane_shift(W[left[i], :, every, :], 1 - cj, -cj)
            SH[2 + i] = lane_shift(W[right[i], :, every, :], (LANES - 1) * cj, LANES * cj - 1)

        def load(k):
            rows = rows_at(SUB * k, SUB)
            return (
                [W[plane, :, rows, :] for plane in own],
                [W[plane, :, rows_at(SUB * k + up, SUB), :] for plane in above],
                [W[plane, :, rows_at(SUB * k + down, SUB), :] for plane in below],
                [X[plane, 0, rows, :] for plane in own],
            )

        change = jnp.zeros((SUB, LANES), F32)
        loaded = load(0)
        count = er // SUB
        for k in range(count):
            rows, flat = rows_at(SUB * k, SUB), slice(SUB * k, SUB * (k + 1))
            w_own, w_above, w_below, field = loaded
            if k < count - 1:
                loaded = load(k + 1)
            w_left = [SH[i, :, flat, :] for i in range(2)]
            w_right = [SH[2 + i, :, flat, :] for i in range(2)]
            inv = [I[plane, :, rows, :] for plane in own]
            stiff = [S[plane, :, rows, :] for plane in own]
            sums = [
                w_above[0] + w_own[2] + w_left[0] + w_own[1],
                w_above[1] + w_own[3] + w_own[0] + w_right[0],
                w_own[0] + w_below[0] + w_left[1] + w_own[3],
                w_own[1] + w_below[1] + w_own[2] + w_right[1],
            ]
            residual = [
                B[own[n], :, rows, :] - (stiff[n] * w_own[n] - sums[n]) for n in range(4)
            ]
            scaled = [stiff[n] * inv[n] for n in range(4)]
            diag = [D[plane, :, rows, :] for plane in own]
            q0 = lax.rsqrt(diag[0])
            l10, l20 = (scaled[0] + scaled[1]) * q0, (scaled[0] + scaled[2]) * q0
            l30 = -((inv[1] + inv[2]) * q0)
            q1 = lax.rsqrt(diag[1] - l10 * l10)
            l21 = (l20 * l10 - (inv[0] + inv[3])) * q1
            l31 = (l30 * l10 + (scaled[1] + scaled[3])) * q1
            q2 = lax.rsqrt(diag[2] - l20 * l20 - l21 * l21)
            l32 = (l30 * l20 + l31 * l21 + (scaled[2] + scaled[3])) * q2
            q3 = lax.rsqrt(diag[3] - l30 * l30 - l31 * l31 - l32 * l32)
            f0 = residual[0] * q0
            f1 = (residual[1] + l10 * f0) * q1
            f2 = (residual[2] + l20 * f0 + l21 * f1) * q2
            f3 = (residual[3] + l30 * f0 + l31 * f1 + l32 * f2) * q3
            z = []
            for n in range(4):
                inner = Z[phase * 4 + n, 0, rows, :]
                if k == 0:
                    inner = jnp.where(low, z_ends[n], inner)
                if k == count - 1:
                    inner = jnp.where(low, inner, z_ends[n])
                z.append(jnp.stack([inner, ZH[slot + n, flat, :]]))
            y0, y1, y2, y3 = f0 + z[0], f1 + z[1], f2 + z[2], f3 + z[3]
            d3 = y3 * q3
            d2 = (y2 + l32 * d3) * q2
            d1 = (y1 + l21 * d2 + l31 * d3) * q1
            d0 = (y0 + l10 * d1 + l20 * d2 + l30 * d3) * q0
            delta = [d0, d1, d2, d3]
            part = 0.0
            for n, f in enumerate((f0, f1, f2, f3)):
                part = part + (z[n][0] * z[n][0] - f[0] * f[0])
            if k == 0:
                part = jnp.where(low, 0.0, part)
            if k == count - 1:
                part = jnp.where(low, part, 0.0)
            change = change + part
            for n, (across, beside) in enumerate(((1, 2), (0, 3), (3, 0), (2, 1))):
                DL[n, :, flat, :] = delta[n]
                X[own[n], 0, rows, :] = field[n] + delta[n][0]
                step = stiff[n] * delta[n] - (delta[across] + delta[beside])
                W[own[n], :, rows, :] = w_own[n] + inv[n] * step
            for i in range(2):
                at = rows_at(SUB * k + up, SUB)
                W[above[i], :, at, :] = w_above[i] - I[above[i], :, at, :] * delta[i]
                at = rows_at(SUB * k + down, SUB)
                W[below[i], :, at, :] = w_below[i] - I[below[i], :, at, :] * delta[2 + i]
        EN[phase + 1] = 0.5 * change
        for i in range(2):
            for plane, n, amount, edge in (
                (left[i], 2 * i, (LANES - 1) * (1 - cj), LANES * (1 - cj) - 1),
                (right[i], 2 * i + 1, cj, cj - 1),
            ):
                value = I[plane, :, every, :] * lane_shift(DL[n], amount, edge)
                W[plane, :, every, :] = W[plane, :, every, :] - value
        halo_noise(jnp.minimum(phase + 1, PHASES - 1))
        return carry

    lax.fori_loop(0, PHASES, run_phase, 0)

    def restore(i, carry):
        for r in (2 * i, 2 * i + 1):
            columns = natural_columns(
                [X[r * CELL + c, 0, rows_at(HC, mr), :] for c in range(CELL)]
            )
            for t, value in enumerate(columns):
                nat[t, pl.ds(r, mr, stride=CELL), :] = value
        return carry

    lax.fori_loop(0, CELL // 2, restore, 0)
    leaving = []
    for t in range(tiles):
        made = pltpu.make_async_copy(
            nat.at[t], out_ref.at[:, pl.ds(t * LANES, LANES)], out_sems.at[t]
        )
        made.start()
        leaving.append(made)

    running = EN[0]
    result = jnp.zeros((1, LANES), F32)
    first_row = lane_iota((1, LANES))
    for phase in range(PHASES):
        if phase:
            running = running + EN[phase]
        total = jnp.sum(jnp.sum(running, axis=0, keepdims=True), axis=1, keepdims=True)
        result = jnp.where(first_row == phase, total, result)
    energy_ref[...] = jnp.broadcast_to(result / nodes, energy_ref.shape)
    for made in leaving:
        made.wait()


def ring(count, step):
    return [(i, (i + step) % count) for i in range(count)]


def estimate(flops):
    return pl.CostEstimate(flops=flops, bytes_accessed=1_000_000, transcendentals=0)


def local(initial_field, information, kappa_squared, lumped_mass, noise_seeds, colour_order):
    chains, tile_rows, tile_cols = initial_field.shape
    row_count, col_count = lax.axis_size("row"), lax.axis_size("col")
    devices = row_count * col_count
    nodes = tile_rows * row_count * tile_cols * col_count
    mr = tile_rows // CELL
    er = mr + 2 * HC
    tiles = tile_cols // LANES
    vmem = pl.BlockSpec(memory_space=pltpu.VMEM)
    hbm = pl.BlockSpec(memory_space=pltpu.HBM)
    params = pltpu.CompilerParams(vmem_limit_bytes=16 * 1024 * 1024)

    def in_hbm(value):
        return pltpu.with_memory_space_constraint(value, pltpu.HBM)

    seeds = in_hbm(jnp.swapaxes(noise_seeds, 3, 4))
    order = in_hbm(colour_order)
    sources = [
        in_hbm(value) for value in (initial_field[0], information, kappa_squared, lumped_mass)
    ]
    rows_shape = jax.ShapeDtypeStruct((4 * HALO, tile_cols), F32)
    cols_shape = jax.ShapeDtypeStruct((4 * CELL * SUB + SUB, LANES), F32)
    up, down, left, right, order_near, seeds_near = pl.pallas_call(
        pack_kernel,
        in_specs=[hbm] * 6,
        out_specs=[vmem] * 6,
        out_shape=[
            rows_shape, rows_shape, cols_shape, cols_shape,
            jax.ShapeDtypeStruct(colour_order.shape, I32),
            jax.ShapeDtypeStruct(seeds.shape, I32),
        ],
        scratch_shapes=[
            pltpu.VMEM((8, tile_rows, LANES), F32),
            pltpu.SemaphoreType.DMA((18,)),
        ],
        compiler_params=params,
        name="pack",
    )(order, seeds, *sources)
    from_right = lax.ppermute(left, "col", ring(col_count, -1))
    from_left = lax.ppermute(right, "col", ring(col_count, 1))
    from_below = lax.ppermute(up, "row", ring(row_count, -1))
    from_above = lax.ppermute(down, "row", ring(row_count, 1))
    planes = CELL * CELL

    def stack(count):
        return (count, 2, er + 2 * BASE, LANES)

    plane_shape = jax.ShapeDtypeStruct(stack(planes), F32)
    noise_shape = jax.ShapeDtypeStruct(stack(PHASES * 4), F32)
    natural_shape = jax.ShapeDtypeStruct((4 * tiles, tile_rows, LANES), F32)
    order_scratch = pltpu.SMEM(colour_order.shape, I32)
    noise, natural = pl.pallas_call(
        functools.partial(noise_kernel, tile_rows, tile_cols),
        in_specs=[vmem] * 2 + [hbm] * 4,
        out_specs=[vmem] * 2,
        out_shape=[noise_shape, natural_shape],
        scratch_shapes=[
            order_scratch,
            pltpu.SMEM(seeds.shape, I32),
            pltpu.SemaphoreType.DMA((4 * tiles + 2,)),
        ],
        compiler_params=params,
        cost_estimate=estimate(4_000_000),
        name="noise",
    )(order_near, seeds_near, *sources)
    corner_shape = jax.ShapeDtypeStruct((3 * SUB, LANES), F32)
    corner_up, corner_down = pl.pallas_call(
        corner_kernel,
        in_specs=[vmem] * 3 + [pl.BlockSpec(memory_space=pl.ANY)],
        out_specs=[vmem] * 2,
        out_shape=[corner_shape, corner_shape],
        compiler_params=params,
        name="corners",
    )(from_right, from_left, left, noise)
    corner_below = lax.ppermute(corner_up, "row", ring(row_count, -1))
    corner_above = lax.ppermute(corner_down, "row", ring(row_count, 1))
    state = pl.pallas_call(
        functools.partial(planes_kernel, tile_rows, tile_cols),
        in_specs=[vmem] * 3,
        out_specs=[vmem] * 4,
        out_shape=[plane_shape] * 4,
        compiler_params=params,
        cost_estimate=estimate(4_000_000),
        name="planes",
    )(natural, from_right, from_left)
    result, energy, *_ = pl.pallas_call(
        functools.partial(sweep_kernel, tile_rows, tile_cols, nodes),
        in_specs=[vmem] * 12,
        out_specs=[hbm] + [vmem] * 5,
        out_shape=[
            jax.ShapeDtypeStruct((tile_rows, tile_cols), F32),
            jax.ShapeDtypeStruct((devices, LANES), F32),
        ]
        + [plane_shape] * 4,
        input_output_aliases={1 + i: 2 + i for i in range(4)},
        scratch_shapes=[
            pltpu.VMEM((4 * tiles, 2 * HALO, LANES), F32),
            pltpu.VMEM(stack(planes), F32),
            pltpu.VMEM(stack(planes), F32),
            pltpu.VMEM((4, 2, er, LANES), F32),
            pltpu.VMEM((4, 2, er, LANES), F32),
            pltpu.VMEM((8, er, LANES), F32),
            pltpu.VMEM((8, SUB, LANES), F32),
            pltpu.VMEM((PHASES + 1, SUB, LANES), F32),
            pltpu.VMEM((tiles, tile_rows, LANES), F32),
            order_scratch,
            pltpu.SMEM((4, SUB, LANES), F32),
            pltpu.SemaphoreType.DMA((5,)),
            pltpu.SemaphoreType.DMA((tiles,)),
        ],
        compiler_params=params,
        cost_estimate=estimate(8_000_000),
        name="sweeps",
    )(
        order_near, *state, noise,
        from_below, from_above, from_right, from_left, corner_below, corner_above,
    )
    shared = lax.all_to_all(energy, AXES, 0, 0, tiled=True)
    energies = jnp.sum(shared, axis=0)[:PHASES].reshape(SWEEPS, COLOURS, chains)
    return (result[None], energies)


def solution(mesh):
    placed = (
        P(None, "row", "col"),
        P("row", "col"),
        P("row", "col"),
        P("row", "col"),
        P("row", "col", None, None, None),
        P(),
    )
    return jax.shard_map(
        local, mesh=mesh, in_specs=placed, out_specs=(P(None, "row", "col"), P()), check_vma=False
    )
```

```python
import functools

import jax
import jax.numpy as jnp
from jax import lax
from jax.experimental import pallas as pl
from jax.experimental.pallas import tpu as pltpu
from jax.sharding import PartitionSpec as P


SWEEPS = 2
COLOURS = 4
PHASES = SWEEPS * COLOURS
HALO = 2 * PHASES
CELL = 4
HC = HALO // CELL
LANES = 128
SUB = 8
GROUP = LANES // CELL
AXES = ("row", "col")
F32 = jnp.float32
I32 = jnp.int32

unit_step = 1.0 / 8388608.0
mix_factor = 73244475
SEED_BASE = 32768
NOISE_SPLIT = 6

SIN_COEFFS = (
    -6.283185159611163,
    41.3416549293435,
    -81.60099819261265,
    76.54965682062002,
    -39.535813711455276,
)


def lane_iota(shape):
    return lax.broadcasted_iota(I32, shape, len(shape) - 1)


def sub_iota(shape):
    return lax.broadcasted_iota(I32, shape, len(shape) - 2)


def lane_gather(value, index):
    return jnp.take_along_axis(value, index, axis=1, mode="promise_in_bounds")


def lroll(value, amount):
    amount = amount % value.shape[1]
    return pltpu.roll(value, amount, 1) if amount else value


SLOT = 8


def slot_gather(value, left):
    wide = lane_iota(value.shape)
    at = (wide + SLOT // 2) % LANES if left else wide
    index = CELL * (at % CELL) + (at % GROUP) // SLOT
    return lane_gather(value, index + (LANES - HALO if left else 0))


def lane_group(left):
    lane = lane_iota((SUB, LANES))
    return ((lane + SLOT // 2) % LANES if left else lane) // GROUP


def pick_group(group, values):
    result = values[0]
    for g in range(1, CELL):
        result = jnp.where(group == g, values[g], result)
    return result


def join_sides(right, left):
    return jnp.where(lane_iota(right.shape) % SLOT < SLOT // 2, right, left)


def pack_kernel(order_ref, seeds_ref, *refs):
    sources, (up_ref, down_ref, left_ref, right_ref, order_out, seeds_buf) = refs[:4], refs[4:10]
    nat, sems = refs[10:]
    rows, cols = sources[0].shape
    mr = rows // CELL
    tiles = cols // LANES
    copies = []

    def copy(source, target):
        made = pltpu.make_async_copy(source, target, sems.at[len(copies)])
        made.start()
        copies.append(made)

    def page(a, t):
        copy(sources[a].at[:, pl.ds(t * LANES, LANES)], nat.at[a * tiles + t])

    copy(seeds_ref, seeds_buf)
    copy(order_ref, order_out)
    for a in range(4):
        page(a, 0)
        page(a, tiles - 1)
    for a, source in enumerate(sources):
        copy(source.at[pl.ds(0, HALO)], up_ref.at[pl.ds(a * HALO, HALO)])
        copy(source.at[pl.ds(rows - HALO, HALO)], down_ref.at[pl.ds(a * HALO, HALO)])
    needed = len(copies)
    for a in range(4):
        for t in range(1, tiles - 1):
            page(a, t)
    for made in copies[:needed]:
        made.wait()
    for sweep in range(SWEEPS):
        seeds = seeds_buf[0, 0, sweep]
        high = (seeds // SEED_BASE).astype(F32)
        low = (seeds % SEED_BASE).astype(F32)
        for out in (left_ref, right_ref):
            base = out.shape[0] - SUB
            out[base + sweep : base + sweep + 1, 0:COLOURS] = high
            out[base + SWEEPS + sweep : base + SWEEPS + sweep + 1, 0:COLOURS] = low

    def pack(a, carry):
        for edge, out in ((0, left_ref), (1, right_ref)):
            group = lane_group(edge == 1)
            for r in range(CELL):
                value = slot_gather(
                    nat[a * tiles + edge * (tiles - 1), pl.ds(r, mr, stride=CELL), :], edge == 1
                )
                parts = [value[SUB * g : SUB * (g + 1)] for g in range(CELL)]
                at = pl.multiple_of((a * CELL + r) * SUB, SUB)
                out[pl.ds(at, SUB), :] = pick_group(group, parts)
        return carry

    lax.fori_loop(0, 4, pack, 0)
    for made in copies[needed:]:
        made.wait()


def half_turn(value):
    return pltpu.roll(value, SUB // 2, 0)


def corner_kernel(right_ref, left_ref, own_ref, after_ref, up_ref, down_ref):
    del after_ref
    group = lane_group(True)
    low = sub_iota((SUB, LANES)) < HC
    ups, downs = [], []
    for a in range(4):
        sides = []
        for r in range(CELL):
            rows = slice((a * CELL + r) * SUB, (a * CELL + r + 1) * SUB)
            sides.append(join_sides(right_ref[rows, :], left_ref[rows, :]))
        ups.append(pick_group(group, [lroll(v, GROUP * r) for r, v in enumerate(sides)]))
        downs.append(pick_group(group, [lroll(v, GROUP * (r + 1)) for r, v in enumerate(sides)]))
    for pair in range(2):
        rows = slice(pair * SUB, (pair + 1) * SUB)
        up_ref[rows, :] = jnp.where(low, ups[2 * pair], half_turn(ups[2 * pair + 1]))
        down_ref[rows, :] = jnp.where(low, half_turn(downs[2 * pair + 1]), downs[2 * pair])
    base = right_ref.shape[0] - SUB
    for out in (up_ref, down_ref):
        for i, source in enumerate((right_ref, left_ref, own_ref)):
            out[2 * SUB : 2 * SUB + SUB // 2, i * SUB : i * SUB + COLOURS] = source[
                base : base + SUB // 2, 0:COLOURS
            ]


def scramble(hashed):
    sixteen = jnp.full_like(hashed, 16)
    hashed = hashed ^ lax.shift_right_logical(hashed, sixteen)
    hashed = hashed * mix_factor
    hashed = hashed ^ lax.shift_right_logical(hashed, sixteen)
    hashed = hashed * mix_factor
    return hashed ^ lax.shift_right_logical(hashed, sixteen)


def gaussian(first):
    nine = jnp.full_like(first, 9)
    one = lax.shift_right_logical(scramble(first), nine).astype(F32)
    two = lax.shift_right_logical(scramble(first + 1), nine).astype(F32)
    u1 = (one + 1.0) * unit_step
    v = 0.25 - jnp.abs(two * unit_step - 0.5)
    square = v * v
    poly = jnp.full_like(v, SIN_COEFFS[-1])
    for coeff in SIN_COEFFS[-2::-1]:
        poly = poly * square + coeff
    square = -2.0 * jnp.log(u1)
    return square * lax.rsqrt(jnp.maximum(square, 1e-30)) * (v * poly)


BASE = SUB


def rows_at(first, count):
    return pl.ds(BASE + first, count)


def lane_shift(value, amount, edge):
    moved = pltpu.roll(value, amount, 2)
    other = jnp.concatenate([moved[1:2], moved[0:1]], axis=0)
    return jnp.where(lane_iota(value.shape) == edge, other, moved)


def fold(value):
    count = value.shape[0]
    sub = sub_iota((SUB, LANES))
    total = jnp.where(sub >= HC, value[0:SUB], value[count - SUB : count])
    for top in range(SUB, count - SUB, SUB):
        total = total + value[top : top + SUB]
    return total


def gather_cells(value, t):
    wide = lane_iota(value.shape)
    column = (wide // GROUP + CELL - t) % CELL
    return lane_gather(value, CELL * (wide % GROUP) + column)


def scatter_cells(value, t):
    wide = lane_iota(value.shape)
    return lane_gather(value, GROUP * ((wide % CELL + t) % CELL) + wide // CELL)


def column_planes(pieces):
    group = lane_iota(pieces[0].shape) // GROUP
    turned = [gather_cells(piece, t) for t, piece in enumerate(pieces)]
    return [
        lroll(pick_group(group, [turned[(g - c) % CELL] for g in range(CELL)]), -GROUP * c)
        for c in range(CELL)
    ]


def natural_columns(planes):
    group = lane_iota(planes[0].shape) // GROUP
    turned = [lroll(plane, GROUP * c) for c, plane in enumerate(planes)]
    return [
        scatter_cells(pick_group(group, [turned[(g - t) % CELL] for g in range(CELL)]), t)
        for t in range(CELL)
    ]


def put_ends(ref, plane, half, value):
    count = ref.shape[2] - 2 * BASE
    ref[plane, half, pl.ds(BASE + count - HC, HC), :] = value[0:HC]
    ref[plane, half, pl.ds(BASE, HC), :] = value[HC:SUB]


def node_offsets(tile_cols, row_cell, col_cell):
    return 2 * CELL * tile_cols * row_cell + 2 * CELL * col_cell


def phase_extra(colour, n, tile_cols):
    row, col = 2 * (colour // 2) + n // 2, 2 * (colour % 2) + n % 2
    return 2 * (row * tile_cols + col)


def noise_kernel(tile_rows, tile_cols, first, last, order_ref, seeds_ref, *refs):
    Z, order, seeds, sems = refs[-4:]
    mr = tile_rows // CELL
    copies = []
    for at, (source, target) in enumerate(((order_ref, order), (seeds_ref, seeds))):
        made = pltpu.make_async_copy(source, target, sems.at[at])
        made.start()
        copies.append(made)
    for made in copies:
        made.wait()
    offset_main = node_offsets(tile_cols, sub_iota((mr, LANES)), lane_iota((mr, LANES)))

    def noise_phase(phase, carry):
        own = seeds[0, 0, phase // COLOURS, 0, phase % COLOURS]
        colour = order[phase % COLOURS]
        for n in range(4):
            start = own + phase_extra(colour, n, tile_cols)
            Z[phase * 4 + n, 0, rows_at(HC, mr), :] = gaussian(offset_main + start)
        return carry

    lax.fori_loop(first, last, noise_phase, 0)


def planes_kernel(tile_rows, tile_cols, nat, right_ref, left_ref, X, B, S, I):
    mr = tile_rows // CELL
    tiles = tile_cols // LANES

    def row(r, carry):
        inner, outer = [], []
        for a in range(4):
            inner.append(
                column_planes(
                    [nat[a * tiles + t, pl.ds(r, mr, stride=CELL), :] for t in range(tiles)]
                )
            )
            rows = pl.ds(pl.multiple_of((a * CELL + r) * SUB, SUB), SUB)
            side = join_sides(right_ref[rows, :], left_ref[rows, :])
            outer.append([lroll(side, -SLOT * slot) for slot in range(LANES // SLOT)])
        for c in range(CELL):
            plane = r * CELL + c
            X[plane, 0, rows_at(HC, mr), :] = inner[0][c]
            B[plane, 0, rows_at(HC, mr), :] = inner[1][c]
            S[plane, 0, rows_at(HC, mr), :] = inner[2][c] * inner[3][c] + 4.0
            I[plane, 0, rows_at(HC, mr), :] = 1.0 / inner[3][c]
            for g in range(CELL):
                slot = CELL * g + c
                at = rows_at(HC + SUB * g, SUB)
                X[plane, 1, at, :] = outer[0][slot]
                B[plane, 1, at, :] = outer[1][slot]
                S[plane, 1, at, :] = outer[2][slot] * outer[3][slot] + 4.0
                I[plane, 1, at, :] = 1.0 / outer[3][slot]
        return carry

    lax.fori_loop(0, CELL, row, 0)


def sweep_kernel(
    tile_rows, tile_cols, nodes,
    order_ref, x_in, b_in, s_in, i_in, Z,
    below_ref, above_ref, right_ref, left_ref, cbelow_ref, cabove_ref,
    out_ref, energy_ref, X, B, S, I,
    strip, W, D, SH, DL, ZH, ZE, EN, nat, order, around, sems, out_sems,
):
    del x_in, b_in, s_in, i_in
    copies = []

    def copy(source, target):
        made = pltpu.make_async_copy(source, target, sems.at[len(copies)])
        made.start()
        copies.append(made)

    copy(order_ref, order)
    for at, ref in enumerate((right_ref, left_ref, cabove_ref, cbelow_ref)):
        copy(ref.at[pl.ds(ref.shape[0] - SUB, SUB)], around.at[at])
    mr = tile_rows // CELL
    er = mr + 2 * HC
    tiles = tile_cols // LANES
    lane = lane_iota((SUB, LANES))
    sub = sub_iota((SUB, LANES))
    low = sub < HC

    corner = []
    for pair in range(2):
        at = slice(pair * SUB, (pair + 1) * SUB)
        under, over = cbelow_ref[at, :], cabove_ref[at, :]
        corner.append(jnp.where(low, under, over))
        corner.append(half_turn(jnp.where(low, over, under)))

    def strips(a, carry):
        for t in range(tiles):
            lanes = slice(t * LANES, (t + 1) * LANES)
            at = pl.ds(pl.multiple_of(a * HALO, HALO), HALO)
            for start, source in ((0, below_ref), (HALO, above_ref)):
                strip[a * tiles + t, start : start + HALO, :] = source[at, lanes]
        return carry

    lax.fori_loop(0, 4, strips, 0)

    def ends(r, carry):
        inner = [
            column_planes(
                [strip[a * tiles + t, pl.ds(r, SUB, stride=CELL), :] for t in range(tiles)]
            )
            for a in range(4)
        ]
        for c in range(CELL):
            plane = r * CELL + c
            amount = (2 * LANES - GROUP * r - SLOT * c) % LANES
            outer = [pltpu.roll(value, amount, 1) for value in carry]
            for half, value in enumerate(([v[c] for v in inner], outer)):
                put_ends(X, plane, half, value[0])
                put_ends(B, plane, half, value[1])
                put_ends(S, plane, half, value[2] * value[3] + 4.0)
                put_ends(I, plane, half, 1.0 / value[3])
        return carry

    lax.fori_loop(0, CELL // 2, lambda i, carry: ends(2 * i + 1, ends(2 * i, carry)), tuple(corner))

    every = rows_at(0, er)

    def start(r, energy):
        above, up = (r + CELL - 1) % CELL, jnp.where(r == 0, -1, 0)
        below, down = (r + 1) % CELL, jnp.where(r == CELL - 1, 1, 0)
        field = [X[r * CELL + c, :, every, :] for c in range(CELL)]
        inv = [I[r * CELL + c, :, every, :] for c in range(CELL)]

        def around_sum(ref, value, c):
            left = value[c - 1] if c else lane_shift(value[CELL - 1], 1, 0)
            right = value[c + 1] if c < CELL - 1 else lane_shift(value[0], LANES - 1, LANES - 1)
            return (
                ref[above * CELL + c, :, rows_at(up, er), :]
                + ref[below * CELL + c, :, rows_at(down, er), :]
                + left
                + right
            )

        for c in range(CELL):
            plane = r * CELL + c
            stiff = S[plane, :, every, :]
            first = stiff * field[c] - around_sum(X, field, c)
            scaled = inv[c] * first
            W[plane, :, every, :] = scaled
            D[plane, :, every, :] = stiff * stiff * inv[c] + around_sum(I, inv, c)
            part = 0.5 * scaled[0] * first[0] - B[plane, 0, every, :] * field[c][0]
            energy = energy + fold(part)
        return energy

    EN[0] = lax.fori_loop(0, CELL, start, jnp.zeros((SUB, LANES), F32))

    for made in copies:
        made.wait()
    spot = lane % GROUP
    is_right = spot < GROUP // 2
    in_right_corner = (lane >= 2 * HC) & (lane < 3 * HC)
    in_left_corner = (lane >= HC) & (lane < 2 * HC)
    end_cell = jnp.where(low, sub, sub + mr - 2 * HC)
    side_row = SUB * jnp.where(is_right, lane // GROUP, (lane // GROUP + 1) % CELL) + sub
    side_row = jnp.where(in_right_corner | in_left_corner, end_cell, side_row)
    side_col = jnp.where(is_right, spot, spot + LANES - GROUP)
    side_col = jnp.where(in_right_corner, lane - 2 * HC, side_col)
    side_col = jnp.where(in_left_corner, lane + LANES - 2 * HC, side_col)
    offset_side = node_offsets(tile_cols, side_row, side_col)
    offset_ends = node_offsets(tile_cols, end_cell, lane)

    def halo_noise(phase):
        sweep, k = phase // COLOURS, phase % COLOURS
        colour = order[k]

        def seed(at, block):
            high = around[at, sweep, block * SUB + k].astype(I32)
            return high * SEED_BASE + around[at, SWEEPS + sweep, block * SUB + k].astype(I32)

        ends_seed = offset_ends + jnp.where(low, seed(3, 2), seed(2, 2))
        side_seed = jnp.where(is_right, seed(0, 0), seed(1, 0))
        ends = jnp.where(low, seed(3, 0), seed(2, 0))
        side_seed = jnp.where(in_right_corner, ends, side_seed)
        ends = jnp.where(low, seed(3, 1), seed(2, 1))
        side_seed = offset_side + jnp.where(in_left_corner, ends, side_seed)
        for n in range(4):
            extra = phase_extra(colour, n, tile_cols)
            at = (phase % 2) * 4 + n
            ZE[at] = half_turn(gaussian(ends_seed + extra))
            value = gaussian(side_seed + extra)
            for g in range(mr // SUB):
                ZH[at, HC + SUB * g : HC + SUB * (g + 1), :] = lroll(value, -GROUP * g)
            value = lroll(value, -2 * HC)
            ZH[at, er - HC : er, :] = value[0:HC]
            ZH[at, 0:HC, :] = value[HC:SUB]

    halo_noise(jnp.int32(0))

    def run_phase(phase, carry):
        colour = order[phase % COLOURS]
        ci, cj = colour // 2, colour % 2
        r0, c0 = 2 * ci, 2 * cj
        slot = (phase % 2) * 4
        z_ends = [ZE[slot + n] for n in range(4)]
        own = [(r0 + n // 2) * CELL + c0 + n % 2 for n in range(4)]
        above, up = (r0 + CELL - 1) % CELL, ci - 1
        below, down = (r0 + 2) % CELL, ci
        left, right = (c0 + CELL - 1) % CELL, (c0 + 2) % CELL
        above = [above * CELL + c0 + i for i in range(2)]
        below = [below * CELL + c0 + i for i in range(2)]
        left = [(r0 + i) * CELL + left for i in range(2)]
        right = [(r0 + i) * CELL + right for i in range(2)]
        for i in range(2):
            SH[i] = lane_shift(W[left[i], :, every, :], 1 - cj, -cj)
            SH[2 + i] = lane_shift(W[right[i], :, every, :], (LANES - 1) * cj, LANES * cj - 1)

        def load(k):
            rows = rows_at(SUB * k, SUB)
            return (
                [W[plane, :, rows, :] for plane in own],
                [W[plane, :, rows_at(SUB * k + up, SUB), :] for plane in above],
                [W[plane, :, rows_at(SUB * k + down, SUB), :] for plane in below],
                [X[plane, 0, rows, :] for plane in own],
            )

        change = jnp.zeros((SUB, LANES), F32)
        loaded = load(0)
        count = er // SUB
        for k in range(count):
            rows, flat = rows_at(SUB * k, SUB), slice(SUB * k, SUB * (k + 1))
            w_own, w_above, w_below, field = loaded
            if k < count - 1:
                loaded = load(k + 1)
            w_left = [SH[i, :, flat, :] for i in range(2)]
            w_right = [SH[2 + i, :, flat, :] for i in range(2)]
            inv = [I[plane, :, rows, :] for plane in own]
            stiff = [S[plane, :, rows, :] for plane in own]
            sums = [
                w_above[0] + w_own[2] + w_left[0] + w_own[1],
                w_above[1] + w_own[3] + w_own[0] + w_right[0],
                w_own[0] + w_below[0] + w_left[1] + w_own[3],
                w_own[1] + w_below[1] + w_own[2] + w_right[1],
            ]
            residual = [
                B[own[n], :, rows, :] - (stiff[n] * w_own[n] - sums[n]) for n in range(4)
            ]
            scaled = [stiff[n] * inv[n] for n in range(4)]
            diag = [D[plane, :, rows, :] for plane in own]
            q0 = lax.rsqrt(diag[0])
            l10, l20 = (scaled[0] + scaled[1]) * q0, (scaled[0] + scaled[2]) * q0
            l30 = -((inv[1] + inv[2]) * q0)
            q1 = lax.rsqrt(diag[1] - l10 * l10)
            l21 = (l20 * l10 - (inv[0] + inv[3])) * q1
            l31 = (l30 * l10 + (scaled[1] + scaled[3])) * q1
            q2 = lax.rsqrt(diag[2] - l20 * l20 - l21 * l21)
            l32 = (l30 * l20 + l31 * l21 + (scaled[2] + scaled[3])) * q2
            q3 = lax.rsqrt(diag[3] - l30 * l30 - l31 * l31 - l32 * l32)
            f0 = residual[0] * q0
            f1 = (residual[1] + l10 * f0) * q1
            f2 = (residual[2] + l20 * f0 + l21 * f1) * q2
            f3 = (residual[3] + l30 * f0 + l31 * f1 + l32 * f2) * q3
            z = []
            for n in range(4):
                inner = Z[phase * 4 + n, 0, rows, :]
                if k == 0:
                    inner = jnp.where(low, z_ends[n], inner)
                if k == count - 1:
                    inner = jnp.where(low, inner, z_ends[n])
                z.append(jnp.stack([inner, ZH[slot + n, flat, :]]))
            y0, y1, y2, y3 = f0 + z[0], f1 + z[1], f2 + z[2], f3 + z[3]
            d3 = y3 * q3
            d2 = (y2 + l32 * d3) * q2
            d1 = (y1 + l21 * d2 + l31 * d3) * q1
            d0 = (y0 + l10 * d1 + l20 * d2 + l30 * d3) * q0
            delta = [d0, d1, d2, d3]
            part = 0.0
            for n, f in enumerate((f0, f1, f2, f3)):
                part = part + (z[n][0] * z[n][0] - f[0] * f[0])
            if k == 0:
                part = jnp.where(low, 0.0, part)
            if k == count - 1:
                part = jnp.where(low, part, 0.0)
            change = change + part
            for n, (across, beside) in enumerate(((1, 2), (0, 3), (3, 0), (2, 1))):
                DL[n, :, flat, :] = delta[n]
                X[own[n], 0, rows, :] = field[n] + delta[n][0]
                step = stiff[n] * delta[n] - (delta[across] + delta[beside])
                W[own[n], :, rows, :] = w_own[n] + inv[n] * step
            for i in range(2):
                at = rows_at(SUB * k + up, SUB)
                W[above[i], :, at, :] = w_above[i] - I[above[i], :, at, :] * delta[i]
                at = rows_at(SUB * k + down, SUB)
                W[below[i], :, at, :] = w_below[i] - I[below[i], :, at, :] * delta[2 + i]
        EN[phase + 1] = 0.5 * change
        for i in range(2):
            for plane, n, amount, edge in (
                (left[i], 2 * i, (LANES - 1) * (1 - cj), LANES * (1 - cj) - 1),
                (right[i], 2 * i + 1, cj, cj - 1),
            ):
                value = I[plane, :, every, :] * lane_shift(DL[n], amount, edge)
                W[plane, :, every, :] = W[plane, :, every, :] - value
        halo_noise(jnp.minimum(phase + 1, PHASES - 1))
        return carry

    lax.fori_loop(0, PHASES, run_phase, 0)

    def restore(i, carry):
        for r in (2 * i, 2 * i + 1):
            columns = natural_columns(
                [X[r * CELL + c, 0, rows_at(HC, mr), :] for c in range(CELL)]
            )
            for t, value in enumerate(columns):
                nat[t, pl.ds(r, mr, stride=CELL), :] = value
        return carry

    lax.fori_loop(0, CELL // 2, restore, 0)
    leaving = []
    for t in range(tiles):
        made = pltpu.make_async_copy(
            nat.at[t], out_ref.at[:, pl.ds(t * LANES, LANES)], out_sems.at[t]
        )
        made.start()
        leaving.append(made)

    running = EN[0]
    result = jnp.zeros((1, LANES), F32)
    first_row = lane_iota((1, LANES))
    for phase in range(PHASES):
        if phase:
            running = running + EN[phase]
        total = jnp.sum(jnp.sum(running, axis=0, keepdims=True), axis=1, keepdims=True)
        result = jnp.where(first_row == phase, total, result)
    energy_ref[...] = jnp.broadcast_to(result / nodes, energy_ref.shape)
    for made in leaving:
        made.wait()


def ring(count, step):
    return [(i, (i + step) % count) for i in range(count)]


def estimate(flops):
    return pl.CostEstimate(flops=flops, bytes_accessed=1_000_000, transcendentals=0)


def local(initial_field, information, kappa_squared, lumped_mass, noise_seeds, colour_order):
    chains, tile_rows, tile_cols = initial_field.shape
    row_count, col_count = lax.axis_size("row"), lax.axis_size("col")
    devices = row_count * col_count
    nodes = tile_rows * row_count * tile_cols * col_count
    mr = tile_rows // CELL
    er = mr + 2 * HC
    tiles = tile_cols // LANES
    vmem = pl.BlockSpec(memory_space=pltpu.VMEM)
    hbm = pl.BlockSpec(memory_space=pltpu.HBM)
    params = pltpu.CompilerParams(vmem_limit_bytes=16 * 1024 * 1024)

    def in_hbm(value):
        return pltpu.with_memory_space_constraint(value, pltpu.HBM)

    seeds = in_hbm(jnp.swapaxes(noise_seeds, 3, 4))
    order = in_hbm(colour_order)
    sources = [
        in_hbm(value) for value in (initial_field[0], information, kappa_squared, lumped_mass)
    ]
    rows_shape = jax.ShapeDtypeStruct((4 * HALO, tile_cols), F32)
    natural_shape = jax.ShapeDtypeStruct((4 * tiles, tile_rows, LANES), F32)
    cols_shape = jax.ShapeDtypeStruct((4 * CELL * SUB + SUB, LANES), F32)
    up, down, left, right, order_near, seeds_near, natural = pl.pallas_call(
        pack_kernel,
        in_specs=[hbm] * 6,
        out_specs=[vmem] * 7,
        out_shape=[
            rows_shape, rows_shape, cols_shape, cols_shape,
            jax.ShapeDtypeStruct(colour_order.shape, I32),
            jax.ShapeDtypeStruct(seeds.shape, I32),
            natural_shape,
        ],
        scratch_shapes=[pltpu.SemaphoreType.DMA((10 + 4 * tiles,))],
        compiler_params=params,
        name="pack",
    )(order, seeds, *sources)
    from_right = lax.ppermute(left, "col", ring(col_count, -1))
    from_left = lax.ppermute(right, "col", ring(col_count, 1))
    from_below = lax.ppermute(up, "row", ring(row_count, -1))
    from_above = lax.ppermute(down, "row", ring(row_count, 1))
    planes = CELL * CELL

    def stack(count):
        return (count, 2, er + 2 * BASE, LANES)

    plane_shape = jax.ShapeDtypeStruct(stack(planes), F32)
    noise_shape = jax.ShapeDtypeStruct(stack(PHASES * 4), F32)
    order_scratch = pltpu.SMEM(colour_order.shape, I32)

    def tile_noise(first, last, extra, specs, aliases):
        return pl.pallas_call(
            functools.partial(noise_kernel, tile_rows, tile_cols, first, last),
            in_specs=[vmem] * 2 + specs,
            out_specs=vmem,
            out_shape=noise_shape,
            input_output_aliases=aliases,
            scratch_shapes=[
                order_scratch,
                pltpu.SMEM(seeds.shape, I32),
                pltpu.SemaphoreType.DMA((2,)),
            ],
            compiler_params=params,
            cost_estimate=estimate(2_000_000),
            name="noise",
        )(order_near, seeds_near, *extra)

    anywhere = pl.BlockSpec(memory_space=pl.ANY)
    noise = tile_noise(0, NOISE_SPLIT, (), [], {})
    corner_shape = jax.ShapeDtypeStruct((3 * SUB, LANES), F32)
    corner_up, corner_down = pl.pallas_call(
        corner_kernel,
        in_specs=[vmem] * 3 + [pl.BlockSpec(memory_space=pl.ANY)],
        out_specs=[vmem] * 2,
        out_shape=[corner_shape, corner_shape],
        compiler_params=params,
        name="corners",
    )(from_right, from_left, left, noise)
    corner_below = lax.ppermute(corner_up, "row", ring(row_count, -1))
    corner_above = lax.ppermute(corner_down, "row", ring(row_count, 1))
    noise = tile_noise(NOISE_SPLIT, PHASES, (noise, corner_up), [vmem, anywhere], {2: 0})
    state = pl.pallas_call(
        functools.partial(planes_kernel, tile_rows, tile_cols),
        in_specs=[vmem] * 3,
        out_specs=[vmem] * 4,
        out_shape=[plane_shape] * 4,
        compiler_params=params,
        cost_estimate=estimate(4_000_000),
        name="planes",
    )(natural, from_right, from_left)
    result, energy, *_ = pl.pallas_call(
        functools.partial(sweep_kernel, tile_rows, tile_cols, nodes),
        in_specs=[vmem] * 12,
        out_specs=[hbm] + [vmem] * 5,
        out_shape=[
            jax.ShapeDtypeStruct((tile_rows, tile_cols), F32),
            jax.ShapeDtypeStruct((devices, LANES), F32),
        ]
        + [plane_shape] * 4,
        input_output_aliases={1 + i: 2 + i for i in range(4)},
        scratch_shapes=[
            pltpu.VMEM((4 * tiles, 2 * HALO, LANES), F32),
            pltpu.VMEM(stack(planes), F32),
            pltpu.VMEM(stack(planes), F32),
            pltpu.VMEM((4, 2, er, LANES), F32),
            pltpu.VMEM((4, 2, er, LANES), F32),
            pltpu.VMEM((8, er, LANES), F32),
            pltpu.VMEM((8, SUB, LANES), F32),
            pltpu.VMEM((PHASES + 1, SUB, LANES), F32),
            pltpu.VMEM((tiles, tile_rows, LANES), F32),
            order_scratch,
            pltpu.SMEM((4, SUB, LANES), F32),
            pltpu.SemaphoreType.DMA((5,)),
            pltpu.SemaphoreType.DMA((tiles,)),
        ],
        compiler_params=params,
        cost_estimate=estimate(8_000_000),
        name="sweeps",
    )(
        order_near, *state, noise,
        from_below, from_above, from_right, from_left, corner_below, corner_above,
    )
    shared = lax.all_to_all(energy, AXES, 0, 0, tiled=True)
    energies = jnp.sum(shared, axis=0)[:PHASES].reshape(SWEEPS, COLOURS, chains)
    return (result[None], energies)


def solution(mesh):
    placed = (
        P(None, "row", "col"),
        P("row", "col"),
        P("row", "col"),
        P("row", "col"),
        P("row", "col", None, None, None),
        P(),
    )
    return jax.shard_map(
        local, mesh=mesh, in_specs=placed, out_specs=(P(None, "row", "col"), P()), check_vma=False
    )
```
